32 devices in a mesh: rows: 32 (over z, y, x, core).
Axes of the slice: x: 2, y: 2, z: 4, core: 2. Of those that a mesh axis runs over, the one named last changes fastest.
Arguments:
- source: float32 [64, 131072], P(None, 'rows'), may hold values from -6 to 6
- band_values: float32 [128, 131072], P(None, 'rows'), may hold values from -0.625 to 0.625
- offsets: int32 [128], replicated, may hold values from -128 to 128, as said below
Outputs:
- compressed: float32 [128, 131072], P(None, 'rows')
The draws below stay inside these ranges and needn't reach their ends.
Inputs may be any that keep to these rules, and one draw needn't show every extreme that they name: The 128 offsets are distinct and include both -128 and 128.
All inputs are finite; a program needn't handle non-finite values.
Results may differ from the reference program's by a relative error of at most 0.0003.
Values sent between devices are 32-bit elements; how exact they have to be, the bound alone decides.
A program may use at most 192 MiB of HBM per device.

```python
import jax
import jax.numpy as jnp
from jax import lax

ROWS_DEV = 4096
HB = 128
NB = 128
RB = 64
K1 = 128
K2 = 128
N = 131072
N_ROWS = 32


def draw_offsets(key, part):
    inner = jax.random.permutation(jax.random.fold_in(key, 11), 2 * HB - 1)[:NB - 2] - (HB - 1)
    ends = jnp.array([-HB, HB], jnp.int32)
    return jnp.concatenate([ends, inner.astype(jnp.int32)])


def steps_of(rng, dims, split, smallest, largest):
    gain, own = 1.0, jax.random.fold_in(rng, 6)
    for axis_at, parts in split:
        steps = jnp.exp(jax.random.uniform(jax.random.fold_in(own, axis_at), (parts,), jnp.float32, smallest / len(split), largest / len(split)))
        gain = gain * jnp.repeat(steps, dims[axis_at] // parts).reshape([-1 if axis == axis_at else 1 for axis in range(len(dims))])
    return gain


def bell_draw(own_key, dims, deviation, reach, split=(), kind=jnp.bfloat16):
    values = deviation * jax.random.normal(own_key, dims, jnp.float32)
    if split:
        values = values * steps_of(own_key, dims, split, -0.22, 0.18)
    return jnp.clip(values, -reach, reach).astype(kind)


def setup_inputs(seed: int = 0) -> dict:
    keys = jax.random.split(jax.random.key(seed), 4)
    source = bell_draw(keys[0], (RB, N), 1.0, 6.0, ((1, 32),), jnp.float32)
    band_values = bell_draw(keys[1], (NB, N), (0.5 / NB ** 0.5), 0.625, ((1, 32),), jnp.float32)
    offsets = draw_offsets(jax.random.fold_in(keys[3], 71), 0)
    return dict(source=source, band_values=band_values, offsets=offsets)


def band_blocks(band_values, offsets):
    diagonals = band_values.shape[0]
    blocks = band_values.shape[1] // HB
    values = band_values.reshape(diagonals, blocks, HB).transpose(1, 0, 2)
    within = jnp.arange(HB, dtype=jnp.int32)
    columns = within[None, :] + offsets[:, None].astype(jnp.int32) + HB
    row_index = jnp.broadcast_to(within[None, :], columns.shape)
    blocked = jnp.zeros((blocks, HB, 3 * HB), values.dtype)
    return blocked.at[:, row_index, columns].set(values)

def apply_band(extended, blocked):
    width = extended.shape[0]
    blocks = blocked.shape[0]
    pieces = extended.reshape(width, blocks + 2, HB)
    windows = jnp.concatenate([pieces[:, :-2], pieces[:, 1:-1], pieces[:, 2:]], axis=2)
    result = jnp.einsum('cbj,brj->cbr', windows, blocked, precision=lax.Precision.HIGHEST)
    return result.reshape(width, blocks * HB)

def apply_all(factor, band_values, offsets):
    width = factor.shape[0]
    padded = jnp.pad(factor, ((0, 0), (HB, HB)))

    def slab(index):
        start = (index * ROWS_DEV).astype(jnp.int32)
        anchor = jnp.zeros((), jnp.int32)
        piece = lax.dynamic_slice(padded, (anchor, start), (width, ROWS_DEV + 2 * HB))
        values = lax.dynamic_slice(band_values, (anchor, start), (band_values.shape[0], ROWS_DEV))
        return apply_band(piece, band_blocks(values, offsets))
    stacked = lax.map(slab, jnp.arange(N_ROWS, dtype=jnp.int32))
    return stacked.transpose(1, 0, 2).reshape(width, N_ROWS * ROWS_DEV)

def compress(grammian, retain):
    spanning = grammian[:, :retain]
    coeffs = None
    for repeat in range(2):
        if repeat > 0:
            spanning = jnp.dot(grammian, coeffs.T, precision=lax.Precision.HIGHEST)
        mapped = jnp.dot(grammian, spanning, precision=lax.Precision.HIGHEST)
        metric = jnp.dot(spanning.T, mapped, precision=lax.Precision.HIGHEST)
        metric = 0.5 * (metric + metric.T)
        factor = jnp.linalg.cholesky(metric)
        coeffs = jax.scipy.linalg.solve_triangular(factor, spanning.T, lower=True)
    return coeffs

def reference(source, band_values, offsets):
    total = source.shape[1]
    first = jnp.concatenate([source, apply_all(source, band_values, offsets)], axis=0)
    gram_one = jnp.dot(first, first.T, precision=lax.Precision.HIGHEST) / total
    coeffs_one = compress(gram_one, K1)
    factor = jnp.dot(coeffs_one, first, precision=lax.Precision.HIGHEST)
    once_more = apply_all(factor, band_values, offsets)
    squared = apply_all(once_more, band_values, offsets)
    second = jnp.concatenate([factor, squared], axis=0)
    gram_two = jnp.dot(second, second.T, precision=lax.Precision.HIGHEST) / total
    coeffs_two = compress(gram_two, K2)
    return jnp.dot(coeffs_two, second, precision=lax.Precision.HIGHEST)
```

```python
import functools

import jax
import jax.numpy as jnp
from jax import lax
from jax.experimental import pallas as pl
from jax.experimental.pallas import tpu as pltpu
from jax.sharding import PartitionSpec as P

HB = 128
SUB = 8
LANE = 128
GROUP = 8
MESH = pl.DeviceIdType.MESH
VMEM = pl.BlockSpec(memory_space=pltpu.VMEM)
HBM = pl.BlockSpec(memory_space=pltpu.HBM)
NN = (((1,), (0,)), ((), ()))
NT = (((1,), (1,)), ((), ()))
TN = (((0,), (0,)), ((), ()))
F32 = jnp.float32
BF16 = jnp.bfloat16


def exact(a, b, dims=NN):
    return lax.dot_general(
        a, b, dims, precision=lax.Precision.HIGHEST, preferred_element_type=F32
    )


def bf(a, b, dims=NN):
    return lax.dot_general(a, b, dims, preferred_element_type=F32)


def halves(value):
    high = value.astype(BF16)
    low = (value - high.astype(F32)).astype(BF16)
    return high, low


def block(at, count=1):
    return pl.ds(pl.multiple_of(at * HB, HB), count * HB)


def pack(twice):
    lanes = lax.broadcasted_iota(jnp.int32, twice.shape, 1)
    high = twice.astype(BF16).astype(F32)
    return jnp.where(lanes < LANE // 2, high, twice - high).astype(BF16)


def pack_columns(part):
    return pack(jnp.concatenate([part, part], axis=0).T)


def band_block(values, chosen):
    top, bottom = halves(values.T)
    spread = bf(jnp.concatenate([top, bottom], axis=1), chosen)
    sheared = pltpu.roll(spread, 0, 1, stride=1, stride_axis=0)
    return jnp.concatenate(halves(sheared), axis=1)


def apply_block(bands, z, at):
    window = z[block(at, 3)]
    both = bf(bands[at], jnp.concatenate([window, window], axis=0))
    return pack(both + pltpu.roll(both, LANE // 2, 1))


def fold(square):
    half = LANE // 2
    rows = []
    for i in range(square.shape[0] // LANE):
        row = []
        for k in range(square.shape[1] // LANE):
            part = square[i * LANE : (i + 1) * LANE, k * LANE : (k + 1) * LANE]
            part = part[:half] + part[half:]
            row.append(part[:, :half] + part[:, half:])
        rows.append(jnp.concatenate(row, axis=1))
    return jnp.concatenate(rows, axis=0)


def main_kernel(
    n, source, band, offsets,
    z0, z1, z2, z3, gram,
    sv, bv, ls, hs, lb, hb, bands, mine, got, part, gotb, gathered,
    local_sem, hsend, hrecv, asend, arecv, bsend, brecv, csend, crecv,
):
    me = lax.axis_index("rows")
    right, left = lax.rem(me + 1, n), lax.rem(me + n - 1, n)
    groups = n // GROUP
    team, seat = me // GROUP, lax.rem(me, GROUP)
    local = source.shape[1]
    blocks = local // HB
    deep_s, deep_b = 3 * HB, 2 * HB

    def mate(k):
        return team * GROUP + lax.rem(seat + k, GROUP)

    def peer(k):
        return lax.rem(team + k, groups) * GROUP + seat

    barrier = pltpu.get_barrier_semaphore()

    def greet(device):
        pl.semaphore_signal(barrier, inc=1, device_id=(device,), device_id_type=MESH)

    greet(left)
    greet(right)
    for k in range(1, GROUP):
        greet(mate(k))

    def greet_peer(k, _):
        greet(peer(k))
        return 0

    lax.fori_loop(1, groups, greet_peer, 0)

    loads = []
    cuts = [(source, sv, 0, deep_s), (source, sv, local - deep_s, deep_s),
            (band, bv, 0, deep_b), (band, bv, local - deep_b, deep_b),
            (source, sv, deep_s, local - 2 * deep_s),
            (band, bv, deep_b, local - 2 * deep_b)]
    for index, (src, dst, at, size) in enumerate(cuts):
        where = pl.ds(at, size)
        loads.append(
            pltpu.make_async_copy(src.at[:, where], dst.at[:, where], local_sem.at[index])
        )
    for load in loads:
        load.start()
    for load in loads[:4]:
        load.wait()
    pl.semaphore_wait(barrier, 2 + GROUP - 1 + groups - 1)
    moves = (
        (sv.at[:, pl.ds(local - deep_s, deep_s)], ls, right),
        (sv.at[:, pl.ds(0, deep_s)], hs, left),
        (bv.at[:, pl.ds(local - deep_b, deep_b)], lb, right),
        (bv.at[:, pl.ds(0, deep_b)], hb, left),
    )
    halo = []
    for index, (src, dst, target) in enumerate(moves):
        halo.append(
            pltpu.make_async_remote_copy(
                src_ref=src, dst_ref=dst, send_sem=hsend.at[index],
                recv_sem=hrecv.at[index], device_id=(target,), device_id_type=MESH,
            )
        )
    for copy in halo:
        copy.start()

    diagonals = band.shape[0]
    places = lax.broadcasted_iota(jnp.int32, (3 * HB, diagonals), 0)
    chosen = jnp.where(places == offsets[...] + HB, 1.0, 0.0).T.astype(BF16)
    chosen = jnp.concatenate([chosen, chosen], axis=0)

    loads[4].wait()

    def turn(at, _):
        z0[block(at + 3)] = pack_columns(sv[:, block(at)])
        return 0

    lax.fori_loop(0, blocks, turn, 0, unroll=4)
    loads[5].wait()

    def build(at, _):
        bands[at + 2] = band_block(bv[:, block(at)], chosen)
        return 0

    lax.fori_loop(0, blocks, build, 0, unroll=4)
    for copy in halo:
        copy.wait()
    for k in range(3):
        part_low = jnp.where(me > 0, ls[:, pl.ds(k * HB, HB)], 0.0)
        part_high = jnp.where(me < n - 1, hs[:, pl.ds(k * HB, HB)], 0.0)
        z0[pl.ds(k * HB, HB)] = pack_columns(part_low)
        z0[pl.ds(3 * HB + local + k * HB, HB)] = pack_columns(part_high)
    for k in range(2):
        part_low = jnp.where(me > 0, lb[:, pl.ds(k * HB, HB)], 0.0)
        part_high = jnp.where(me < n - 1, hb[:, pl.ds(k * HB, HB)], 0.0)
        bands[k] = band_block(part_low, chosen)
        bands[2 + blocks + k] = band_block(part_high, chosen)

    def once(at, _):
        z1[block(at)] = apply_block(bands, z0, at)
        return 0

    lax.fori_loop(0, blocks + 4, once, 0, unroll=4)

    def twice(at, _):
        window = z1[block(at, 3)]
        both = bf(bands[at + 1], jnp.concatenate([window, window], axis=0))
        z2[block(at)] = pack(both + pltpu.roll(both, LANE // 2, 1))
        return 0

    lax.fori_loop(0, blocks + 2, twice, 0, unroll=2)

    def thrice(at, _):
        window = z2[block(at, 3)]
        both = bf(bands[at + 2], jnp.concatenate([window, window], axis=0))
        z3[block(at)] = pack(both + pltpu.roll(both, LANE // 2, 1))
        return 0

    lax.fori_loop(0, blocks, thrice, 0, unroll=4)

    def grow(at, sums):
        first = jnp.concatenate([z0[block(2 * at + 3, 2)], z1[block(2 * at + 2, 2)]], axis=1)
        second = jnp.concatenate([z2[block(2 * at + 1, 2)], z3[block(2 * at, 2)]], axis=1)
        a, b, c = sums
        return (a + bf(first, first, TN), b + bf(first, second, TN), c + bf(second, second, TN))

    zero = jnp.zeros((2 * LANE, 2 * LANE), F32)
    sums = lax.fori_loop(0, blocks // 2, grow, (zero, zero, zero))
    stacked = jnp.concatenate([fold(s) for s in sums], axis=0)
    rows = stacked.shape[0] // GROUP
    mine[...] = stacked.reshape(GROUP, rows, LANE)

    def copy_to(src, dst, send, recv, device):
        return pltpu.make_async_remote_copy(
            src_ref=src, dst_ref=dst, send_sem=send, recv_sem=recv,
            device_id=(device,), device_id_type=MESH,
        )

    ahead = []
    for k in range(1, GROUP):
        to = lax.rem(seat + k, GROUP)
        ahead.append(copy_to(mine.at[to], got.at[k], asend.at[k], arecv.at[k], mate(k)))
    for copy in ahead:
        copy.start()
    summed = mine[seat]
    for k, copy in enumerate(ahead):
        copy.wait_recv()
        summed = summed + got[k + 1]
    part[...] = summed

    def across(k):
        return copy_to(part, gotb.at[k], bsend.at[k], brecv.at[k], peer(k))

    def start(k, _):
        across(k).start()
        return 0

    def arrive(k, value):
        across(k).wait_recv()
        return value + gotb[k]

    lax.fori_loop(1, groups, start, 0)
    summed = lax.fori_loop(1, groups, arrive, summed)
    gathered[seat] = summed
    back = []
    for k in range(1, GROUP):
        back.append(copy_to(gathered.at[seat], gathered.at[seat], csend.at[k], crecv.at[k], mate(k)))
    for copy in back:
        copy.start()
    for copy in back:
        copy.wait_recv()
    gram[...] = gathered[...]
    for copy in ahead + back:
        copy.wait_send()

    def sent(k, _):
        across(k).wait_send()
        return 0

    lax.fori_loop(1, groups, sent, 0)


def make_main(source, band, offsets):
    n = lax.axis_size("rows")
    width, local = source.shape
    diagonals = band.shape[0]
    blocks = local // HB
    groups = n // GROUP
    rows = 3 * LANE // GROUP
    dma = pltpu.SemaphoreType.DMA
    shape = jax.ShapeDtypeStruct
    vm = pltpu.VMEM
    return pl.pallas_call(
        functools.partial(main_kernel, n),
        out_shape=[
            shape((local + 6 * HB, LANE), BF16),
            shape((local + 4 * HB, LANE), BF16),
            shape((local + 2 * HB, LANE), BF16),
            shape((local, LANE), BF16),
            shape((GROUP, rows, LANE), F32),
        ],
        in_specs=[HBM, HBM, VMEM],
        out_specs=[VMEM] * 5,
        scratch_shapes=[
            vm((width, local), F32),
            vm((diagonals, local), F32),
            vm((width, 3 * HB), F32), vm((width, 3 * HB), F32),
            vm((diagonals, 2 * HB), F32), vm((diagonals, 2 * HB), F32),
            vm((blocks + 4, HB, 6 * HB), BF16),
            vm((GROUP, rows, LANE), F32),
            vm((GROUP, rows, LANE), F32),
            vm((rows, LANE), F32),
            vm((groups, rows, LANE), F32),
            vm((GROUP, rows, LANE), F32),
            dma((6,)), dma((4,)), dma((4,)),
            dma((GROUP,)), dma((GROUP,)), dma((groups,)), dma((groups,)),
            dma((GROUP,)), dma((GROUP,)),
        ],
        compiler_params=pltpu.CompilerParams(
            collective_id=0, has_side_effects=True, vmem_limit_bytes=40 << 20
        ),
    )(source, band, offsets.reshape(1, diagonals))


def splat(value):
    return jnp.broadcast_to(value, (SUB, LANE))


def eliminate(metric, right):
    tiles = metric.shape[0] // SUB
    part = [slice(SUB * t, SUB * t + SUB) for t in range(tiles)]
    state = [[metric[part[t]], right[part[t]]] for t in range(tiles)]
    rows = lax.broadcasted_iota(jnp.int32, (SUB, LANE), 0)
    solved = []
    steps = range(SUB)
    for t0 in range(tiles):
        at = SUB * t0
        core = {
            (i, k): splat(state[t0][0][i : i + 1, at + k : at + k + 1])
            for i in steps
            for k in range(i, SUB)
        }
        pivots = [[splat(half[i : i + 1]) for half in state[t0]] for i in steps]
        inverse = []
        for i in steps:
            inverse.append(1.0 / core[i, i])
            for k in range(i + 1, SUB):
                ratio = core[i, k] * inverse[i]
                for m in range(k, SUB):
                    core[k, m] = core[k, m] - ratio * core[i, m]
                pivots[k] = [p - ratio * q for p, q in zip(pivots[k], pivots[i])]
        result = jnp.zeros((SUB, LANE), F32)
        for i in steps:
            result = jnp.where(rows == i, pivots[i][1] * lax.rsqrt(core[i, i]), result)
        solved.append(result)
        for t in range(t0 + 1, tiles):
            scaled = []
            for k in steps:
                column = splat(state[t][0][:, at + k : at + k + 1])
                for i in range(k):
                    column = column - scaled[i] * core[i, k]
                scaled.append(column * inverse[k])
            for half in range(2):
                value = state[t][half]
                for k in steps:
                    value = value - scaled[k] * pivots[k][half]
                state[t][half] = value
    return jnp.concatenate(solved, axis=0)


def compress(grammian, retain):
    spanning = grammian[:retain]
    wide = spanning.shape[1] > retain
    across = lax.broadcasted_iota(jnp.int32, (retain, retain), 1)
    down = lax.broadcasted_iota(jnp.int32, (retain, retain), 0)
    unit = jnp.where(across == down, 1.0, 0.0)
    coeffs = None
    for repeat in range(2):
        if repeat > 0:
            spanning = exact(coeffs, grammian)
        metric = exact(exact(spanning, grammian), spanning, NT)
        metric = 0.5 * (metric + metric.T)
        if wide:
            coeffs = exact(eliminate(metric, unit), spanning)
        else:
            coeffs = eliminate(metric, spanning)
    return coeffs


def last_kernel(total, gram, z0, z1, z2, z3, out, tile, sem):
    keep = LANE
    every = gram[...].reshape(3 * LANE, LANE) * (1.0 / total)
    own, cross, far = every[:keep], every[keep : 2 * keep], every[2 * keep :]
    once = compress(own, keep)
    cross = exact(exact(once, cross), once, NT)
    far = exact(exact(once, far), once, NT)
    across = lax.broadcasted_iota(jnp.int32, (keep, keep), 1)
    down = lax.broadcasted_iota(jnp.int32, (keep, keep), 0)
    unit = jnp.where(across == down, 1.0, 0.0)
    top = jnp.concatenate([unit, cross], axis=1)
    bottom = jnp.concatenate([cross.T, far], axis=1)
    again = compress(jnp.concatenate([top, bottom], axis=0), keep)
    coeffs = jnp.concatenate([exact(again[:, :keep], once), exact(again[:, keep:], once)], axis=1)
    turned = coeffs.T
    half = LANE // 2
    weights = jnp.concatenate(halves(turned), axis=1)
    weights = jnp.concatenate(
        [weights[half * (k // 2) : half * (k // 2) + half] for k in range(8)], axis=0
    )
    local = z3.shape[0]
    count = local // (4 * HB)

    def store(at):
        where = pl.ds(pl.multiple_of(at * 4 * HB, 4 * HB), 4 * HB)
        return pltpu.make_async_copy(tile.at[at], out.at[:, where], sem.at[at])

    def step(at, _):
        where = [pl.ds(pl.multiple_of(at * 4 * HB + k * HB, HB), 4 * HB) for k in (3, 2, 1, 0)]
        lhs = jnp.concatenate([z[w] for z, w in zip((z0, z1, z2, z3), where)], axis=1)
        both = bf(lhs, weights)
        tile[at] = (both[:, :LANE] + both[:, LANE:]).T
        store(at).start()
        return 0

    lax.fori_loop(0, count, step, 0)

    def finish(at, _):
        store(at).wait()
        return 0

    lax.fori_loop(0, count, finish, 0)


def make_last(z0, z1, z2, z3, gram, total):
    local = z3.shape[0]
    count = local // (4 * HB)
    return pl.pallas_call(
        functools.partial(last_kernel, total),
        out_shape=jax.ShapeDtypeStruct((LANE, local), F32),
        in_specs=[VMEM] * 5,
        out_specs=HBM,
        scratch_shapes=[
            pltpu.VMEM((count, LANE, 4 * HB), F32),
            pltpu.SemaphoreType.DMA((count,)),
        ],
        compiler_params=pltpu.CompilerParams(vmem_limit_bytes=28 << 20),
    )(gram, z0, z1, z2, z3)


def body(source, band_values, offsets):
    total = float(source.shape[1] * lax.axis_size("rows"))
    z0, z1, z2, z3, gram = make_main(source, band_values, offsets)
    return make_last(z0, z1, z2, z3, gram, total)


def solution(mesh):
    placed = (P(None, "rows"), P(None, "rows"), P())
    return jax.shard_map(
        body, mesh=mesh, in_specs=placed, out_specs=P(None, "rows"), check_vma=False
    )
```

```python
import functools

import jax
import jax.numpy as jnp
from jax import lax
from jax.experimental import pallas as pl
from jax.experimental.pallas import tpu as pltpu
from jax.sharding import PartitionSpec as P

HB = 128
SUB = 8
LANE = 128
GROUP = 8
MESH = pl.DeviceIdType.MESH
VMEM = pl.BlockSpec(memory_space=pltpu.VMEM)
HBM = pl.BlockSpec(memory_space=pltpu.HBM)
NN = (((1,), (0,)), ((), ()))
NT = (((1,), (1,)), ((), ()))
TN = (((0,), (0,)), ((), ()))
F32 = jnp.float32
BF16 = jnp.bfloat16


def exact(a, b, dims=NN):
    return lax.dot_general(
        a, b, dims, precision=lax.Precision.HIGHEST, preferred_element_type=F32
    )


def bf(a, b, dims=NN):
    return lax.dot_general(a, b, dims, preferred_element_type=F32)


def halves(value):
    high = value.astype(BF16)
    low = (value - high.astype(F32)).astype(BF16)
    return high, low


def block(at, count=1):
    return pl.ds(pl.multiple_of(at * HB, HB), count * HB)


def pack(twice, flip):
    lanes = lax.broadcasted_iota(jnp.int32, twice.shape, 1)
    high = twice.astype(BF16).astype(F32)
    return jnp.where((lanes < LANE // 2) != flip, high, twice - high).astype(BF16)


def pack_columns(part):
    return pack(jnp.concatenate([part, part], axis=0).T, False)


def band_block(values, chosen):
    top, bottom = halves(values.T)
    spread = bf(jnp.concatenate([top, bottom], axis=1), chosen)
    sheared = pltpu.roll(spread, 0, 1, stride=1, stride_axis=0)
    return jnp.concatenate(halves(sheared), axis=1)


def apply_band(bands, skip, z, out, flip):
    def step(at, _):
        window = z[block(at, 3)]
        both = bf(bands[at + skip], jnp.concatenate([window, window], axis=0))
        out[block(at)] = pack(both + pltpu.roll(both, LANE // 2, 1), flip)
        return 0

    blocks = out.shape[0] // HB
    lax.fori_loop(0, blocks, step, 0, unroll=blocks)


def swap(value):
    return pltpu.roll(value, LANE // 2, 1)


def mixed(even, odd):
    lanes = lax.broadcasted_iota(jnp.int32, even.shape, 1)
    first = lanes < LANE // 2
    return jnp.where(first, even, odd), jnp.where(first, odd, even)


class Total:
    def __init__(self, n, refs):
        self.groups = n // GROUP
        me = lax.axis_index("rows")
        self.team, self.seat = me // GROUP, lax.rem(me, GROUP)
        (self.mine, self.got, self.part, self.gotb, self.gathered,
         self.asend, self.arecv, self.bsend, self.brecv, self.csend, self.crecv) = refs

    def mate(self, k):
        return self.team * GROUP + lax.rem(self.seat + k, GROUP)

    def peer(self, k):
        return lax.rem(self.team + k, self.groups) * GROUP + self.seat

    def copy(self, src, dst, send, recv, device):
        return pltpu.make_async_remote_copy(
            src_ref=src, dst_ref=dst, send_sem=send, recv_sem=recv,
            device_id=(device,), device_id_type=MESH,
        )

    def ahead(self, k):
        to = lax.rem(self.seat + k, GROUP)
        return self.copy(
            self.mine.at[to], self.got.at[k], self.asend.at[k], self.arecv.at[k], self.mate(k)
        )

    def across(self, k):
        return self.copy(
            self.part, self.gotb.at[k], self.bsend.at[k], self.brecv.at[k], self.peer(k)
        )

    def back(self, k):
        own = self.gathered.at[self.seat]
        return self.copy(own, own, self.csend.at[k], self.crecv.at[k], self.mate(k))

    def scatter(self, value):
        self.mine[...] = value.reshape(self.mine.shape)
        for k in range(1, GROUP):
            self.ahead(k).start()

    def middle(self):
        summed = self.mine[self.seat]
        for k in range(1, GROUP):
            self.ahead(k).wait_recv()
            summed = summed + self.got[k]
        self.part[...] = summed

        def start(k, _):
            self.across(k).start()
            return 0

        lax.fori_loop(1, self.groups, start, 0)

    def post(self):
        def arrive(k, value):
            self.across(k).wait_recv()
            return value + self.gotb[k]

        self.gathered[self.seat] = lax.fori_loop(1, self.groups, arrive, self.part[...])
        for k in range(1, GROUP):
            self.back(k).start()

    def finish(self):
        for k in range(1, GROUP):
            self.back(k).wait_recv()
        value = self.gathered[...].reshape(GROUP * self.part.shape[0], LANE)
        for k in range(1, GROUP):
            self.ahead(k).wait_send()
            self.back(k).wait_send()

        def sent(k, _):
            self.across(k).wait_send()
            return 0

        lax.fori_loop(1, self.groups, sent, 0)
        return value

    @staticmethod
    def scratch(n, rows):
        groups, share = n // GROUP, rows // GROUP
        vm, dma = pltpu.VMEM, pltpu.SemaphoreType.DMA
        return [
            vm((GROUP, share, LANE), F32), vm((GROUP, share, LANE), F32),
            vm((share, LANE), F32), vm((groups, share, LANE), F32),
            vm((GROUP, share, LANE), F32),
            dma((GROUP,)), dma((GROUP,)), dma((groups,)), dma((groups,)),
            dma((GROUP,)), dma((GROUP,)),
        ]


def main_kernel(
    n, total, source, band, offsets,
    z0, z1, z2, z3, once, gram,
    sv, bv, ov, ls, hs, lb, hb, bands, local_sem, hsend, hrecv, *totals
):
    me = lax.axis_index("rows")
    right, left = lax.rem(me + 1, n), lax.rem(me + n - 1, n)
    near = Total(n, totals[: len(totals) // 2])
    far = Total(n, totals[len(totals) // 2 :])
    local = source.shape[1]
    blocks = local // HB
    deep_s, deep_b = 3 * HB, 2 * HB
    barrier = pltpu.get_barrier_semaphore()

    def greet(device):
        pl.semaphore_signal(barrier, inc=1, device_id=(device,), device_id_type=MESH)

    def greet_peer(k, _):
        greet(near.peer(k))
        return 0

    greet(left)
    greet(right)
    lax.fori_loop(1, near.groups, greet_peer, 0)
    for k in range(1, GROUP):
        greet(near.mate(k))
    whole = pl.ds(0, offsets.shape[1])
    cuts = [
        (source, sv, pl.ds(0, deep_s)), (source, sv, pl.ds(local - deep_s, deep_s)),
        (band, bv, pl.ds(0, deep_b)), (band, bv, pl.ds(local - deep_b, deep_b)),
        (offsets, ov, whole),
        (source, sv, pl.ds(deep_s, local - 2 * deep_s)),
        (band, bv, pl.ds(deep_b, local - 2 * deep_b)),
    ]
    loads = [
        pltpu.make_async_copy(src.at[:, where], dst.at[:, where], local_sem.at[index])
        for index, (src, dst, where) in enumerate(cuts)
    ]
    for load in loads:
        load.start()
    for load in loads[:4]:
        load.wait()
    pl.semaphore_wait(barrier, 2 + GROUP - 1 + near.groups - 1)
    moves = (
        (sv.at[:, pl.ds(local - deep_s, deep_s)], ls, right),
        (sv.at[:, pl.ds(0, deep_s)], hs, left),
        (bv.at[:, pl.ds(local - deep_b, deep_b)], lb, right),
        (bv.at[:, pl.ds(0, deep_b)], hb, left),
    )
    halo = [
        near.copy(src, dst, hsend.at[index], hrecv.at[index], target)
        for index, (src, dst, target) in enumerate(moves)
    ]
    for copy in halo:
        copy.start()

    loads[4].wait()
    diagonals = band.shape[0]
    places = lax.broadcasted_iota(jnp.int32, (3 * HB, diagonals), 0)
    chosen = jnp.where(places == ov[...] + HB, 1.0, 0.0).T.astype(BF16)
    chosen = jnp.concatenate([chosen, chosen], axis=0)
    loads[5].wait()

    def turn(at, _):
        z0[block(at + 3)] = pack_columns(sv[:, block(at)])
        return 0

    lax.fori_loop(0, blocks, turn, 0, unroll=blocks // 2)
    loads[6].wait()

    def build(at, _):
        bands[at + 2] = band_block(bv[:, block(at)], chosen)
        return 0

    lax.fori_loop(0, blocks, build, 0, unroll=blocks)
    for copy in halo:
        copy.wait_recv()
    for k in range(3):
        part_low = jnp.where(me > 0, ls[:, pl.ds(k * HB, HB)], 0.0)
        part_high = jnp.where(me < n - 1, hs[:, pl.ds(k * HB, HB)], 0.0)
        z0[pl.ds(k * HB, HB)] = pack_columns(part_low)
        z0[pl.ds(3 * HB + local + k * HB, HB)] = pack_columns(part_high)
    for k in range(2):
        part_low = jnp.where(me > 0, lb[:, pl.ds(k * HB, HB)], 0.0)
        part_high = jnp.where(me < n - 1, hb[:, pl.ds(k * HB, HB)], 0.0)
        bands[k] = band_block(part_low, chosen)
        bands[2 + blocks + k] = band_block(part_high, chosen)
    apply_band(bands, 0, z0, z1, True)
    inner0, inner1 = z0[pl.ds(3 * HB, local)], z1[pl.ds(2 * HB, local)]
    high, low = mixed(inner0, inner1)
    product = bf(high, jnp.concatenate([high, low], axis=1), TN)
    cross = swap(product[:, LANE:])
    near.scatter(product[:, :LANE] + cross + cross.T)

    apply_band(bands, 1, z1, z2, False)
    apply_band(bands, 2, z2, z3, True)
    near.middle()
    high, low = mixed(z0[pl.ds(3 * HB, local)], z1[pl.ds(2 * HB, local)])
    high2, low2 = mixed(z2[pl.ds(HB, local)], z3[...])
    product = bf(high2, jnp.concatenate([high, low, high2, low2], axis=1), TN)
    other = bf(high, low2, TN)
    cross = (product[:, :LANE] + swap(product[:, LANE : 2 * LANE])).T + swap(other)
    own = swap(product[:, 3 * LANE :])
    own = product[:, 2 * LANE : 3 * LANE] + own + own.T
    far.scatter(jnp.concatenate([cross, own], axis=0))
    near.post()
    far.middle()
    gram_one = near.finish() * (1.0 / total)
    turned = square_turn(gram_one, gram_one)
    far.post()
    once[...] = square_turn(exact(turned, gram_one), gram_one)
    gram[...] = far.finish() * (1.0 / total)
    for copy in halo:
        copy.wait_send()


def make_main(source, band, offsets, total):
    n = lax.axis_size("rows")
    width, local = source.shape
    diagonals = band.shape[0]
    blocks = local // HB
    dma = pltpu.SemaphoreType.DMA
    shape = jax.ShapeDtypeStruct
    vm = pltpu.VMEM
    return pl.pallas_call(
        functools.partial(main_kernel, n, total),
        out_shape=[
            shape((local + 6 * HB, LANE), BF16),
            shape((local + 4 * HB, LANE), BF16),
            shape((local + 2 * HB, LANE), BF16),
            shape((local, LANE), BF16),
            shape((LANE, LANE), F32),
            shape((2 * LANE, LANE), F32),
        ],
        in_specs=[HBM] * 3,
        out_specs=[VMEM] * 6,
        scratch_shapes=[
            vm((width, local), F32),
            vm((diagonals, local), F32),
            vm((1, diagonals), jnp.int32),
            vm((width, 3 * HB), F32), vm((width, 3 * HB), F32),
            vm((diagonals, 2 * HB), F32), vm((diagonals, 2 * HB), F32),
            vm((blocks + 4, HB, 6 * HB), BF16),
            dma((7,)), dma((4,)), dma((4,)),
        ]
        + Total.scratch(n, LANE)
        + Total.scratch(n, 2 * LANE),
        compiler_params=pltpu.CompilerParams(
            collective_id=0, has_side_effects=True, vmem_limit_bytes=46 << 20
        ),
    )(source, band, offsets.reshape(1, diagonals))


def splat(value):
    return jnp.broadcast_to(value, (SUB, LANE))


def eliminate(metric, right):
    tiles = metric.shape[0] // SUB
    part = [slice(SUB * t, SUB * t + SUB) for t in range(tiles)]
    state = [[metric[part[t]], right[part[t]]] for t in range(tiles)]
    rows = lax.broadcasted_iota(jnp.int32, (SUB, LANE), 0)
    solved = []
    steps = range(SUB)
    for t0 in range(tiles):
        at = SUB * t0
        core = {
            (i, k): splat(state[t0][0][i : i + 1, at + k : at + k + 1])
            for i in steps
            for k in range(i, SUB)
        }
        pivots = [[splat(half[i : i + 1]) for half in state[t0]] for i in steps]
        inverse = []
        for i in steps:
            inverse.append(1.0 / core[i, i])
            for k in range(i + 1, SUB):
                ratio = core[i, k] * inverse[i]
                for m in range(k, SUB):
                    core[k, m] = core[k, m] - ratio * core[i, m]
                pivots[k] = [p - ratio * q for p, q in zip(pivots[k], pivots[i])]
        result = jnp.zeros((SUB, LANE), F32)
        for i in steps:
            result = jnp.where(rows == i, pivots[i][1] * lax.rsqrt(core[i, i]), result)
        solved.append(result)
        for t in range(t0 + 1, tiles):
            scaled = []
            for k in steps:
                column = splat(state[t][0][:, at + k : at + k + 1])
                for i in range(k):
                    column = column - scaled[i] * core[i, k]
                scaled.append(column * inverse[k])
            for half in range(2):
                value = state[t][half]
                for k in steps:
                    value = value - scaled[k] * pivots[k][half]
                state[t][half] = value
    return jnp.concatenate(solved, axis=0)


def square_turn(spanning, grammian):
    return eliminate(exact(exact(spanning, grammian), spanning, NT), spanning)


def last_kernel(once, gram, z0, z1, z2, z3, out, tile, sem):
    keep = LANE
    coeffs = once[...]
    cross, far = gram[:keep], gram[keep:]
    cross = exact(exact(coeffs, cross), coeffs, NT)
    far = exact(exact(coeffs, far), coeffs, NT)
    across = lax.broadcasted_iota(jnp.int32, (keep, keep), 1)
    down = lax.broadcasted_iota(jnp.int32, (keep, keep), 0)
    unit = jnp.where(across == down, 1.0, 0.0)
    span_a = unit + exact(cross, cross, NT)
    span_b = cross + exact(cross, far)
    next_a = span_a + exact(span_b, cross, NT)
    next_b = exact(span_a, cross) + exact(span_b, far)
    metric = exact(next_a, span_a, NT) + exact(next_b, span_b, NT)
    spanning = jnp.concatenate([exact(span_a, coeffs), exact(span_b, coeffs)], axis=1)
    coeffs = exact(eliminate(metric, unit), spanning)
    turned = coeffs.T
    half = LANE // 2
    weights = jnp.concatenate(halves(turned), axis=1)
    weights = jnp.concatenate(
        [weights[half * (k // 2) : half * (k // 2) + half] for k in range(8)], axis=0
    )
    local = z3.shape[0]
    count = local // (4 * HB)

    def store(at):
        where = pl.ds(pl.multiple_of(at * 4 * HB, 4 * HB), 4 * HB)
        return pltpu.make_async_copy(tile.at[at], out.at[:, where], sem.at[at])

    def step(at, _):
        where = [pl.ds(pl.multiple_of(at * 4 * HB + k * HB, HB), 4 * HB) for k in (3, 2, 1, 0)]
        lhs = jnp.concatenate([z[w] for z, w in zip((z0, z1, z2, z3), where)], axis=1)
        both = bf(lhs, weights)
        tile[at] = (both[:, :LANE] + both[:, LANE:]).T
        store(at).start()
        return 0

    lax.fori_loop(0, count, step, 0, unroll=count)

    def finish(at, _):
        store(at).wait()
        return 0

    lax.fori_loop(0, count, finish, 0)


def make_last(once, gram, z0, z1, z2, z3):
    local = z3.shape[0]
    count = local // (4 * HB)
    return pl.pallas_call(
        last_kernel,
        out_shape=jax.ShapeDtypeStruct((LANE, local), F32),
        in_specs=[VMEM] * 6,
        out_specs=HBM,
        scratch_shapes=[
            pltpu.VMEM((count, LANE, 4 * HB), F32),
            pltpu.SemaphoreType.DMA((count,)),
        ],
        compiler_params=pltpu.CompilerParams(vmem_limit_bytes=28 << 20),
    )(once, gram, z0, z1, z2, z3)


def body(source, band_values, offsets):
    total = float(source.shape[1] * lax.axis_size("rows"))
    z0, z1, z2, z3, once, gram = make_main(source, band_values, offsets, total)
    return make_last(once, gram, z0, z1, z2, z3)


def solution(mesh):
    placed = (P(None, "rows"), P(None, "rows"), P())
    return jax.shard_map(
        body, mesh=mesh, in_specs=placed, out_specs=P(None, "rows"), check_vma=False
    )
```

```python
import functools

import jax
import jax.numpy as jnp
from jax import lax
from jax.experimental import pallas as pl
from jax.experimental.pallas import tpu as pltpu
from jax.sharding import PartitionSpec as P

HB = 128
SUB = 8
LANE = 128
GROUP = 8
PIECE = 4 * HB
MESH = pl.DeviceIdType.MESH
VMEM = pl.BlockSpec(memory_space=pltpu.VMEM)
HBM = pl.BlockSpec(memory_space=pltpu.HBM)
NN = (((1,), (0,)), ((), ()))
NT = (((1,), (1,)), ((), ()))
TN = (((0,), (0,)), ((), ()))
F32 = jnp.float32
BF16 = jnp.bfloat16


def exact(a, b, dims=NN):
    return lax.dot_general(
        a, b, dims, precision=lax.Precision.HIGHEST, preferred_element_type=F32
    )


def bf(a, b, dims=NN):
    return lax.dot_general(a, b, dims, preferred_element_type=F32)


def halves(value):
    high = value.astype(BF16)
    low = (value - high.astype(F32)).astype(BF16)
    return high, low


def block(at, count=1):
    return pl.ds(pl.multiple_of(at * HB, HB), count * HB)


def pack(twice, flip):
    lanes = lax.broadcasted_iota(jnp.int32, twice.shape, 1)
    high = twice.astype(BF16).astype(F32)
    return jnp.where((lanes < LANE // 2) != flip, high, twice - high).astype(BF16)


def pack_columns(part):
    return pack(jnp.concatenate([part, part], axis=0).T, False)


def band_block(values, chosen):
    top, bottom = halves(values.T)
    spread = bf(jnp.concatenate([top, bottom], axis=1), chosen)
    sheared = pltpu.roll(spread, 0, 1, stride=1, stride_axis=0)
    return jnp.concatenate(halves(sheared), axis=1)


def apply_band(bands, skip, z, out, flip, start, count):
    def step(k, _):
        at = start + k
        window = z[block(at, 3)]
        both = bf(bands[at + skip], jnp.concatenate([window, window], axis=0))
        out[block(at)] = pack(both + pltpu.roll(both, LANE // 2, 1), flip)
        return 0

    lax.fori_loop(0, count, step, 0, unroll=count)


def swap(value):
    return pltpu.roll(value, LANE // 2, 1)


def mixed(even, odd):
    lanes = lax.broadcasted_iota(jnp.int32, even.shape, 1)
    first = lanes < LANE // 2
    return jnp.where(first, even, odd), jnp.where(first, odd, even)


class Total:
    def __init__(self, n, refs):
        self.groups = n // GROUP
        me = lax.axis_index("rows")
        self.team, self.seat = me // GROUP, lax.rem(me, GROUP)
        (self.mine, self.got, self.part, self.gotb, self.gathered,
         self.asend, self.arecv, self.bsend, self.brecv, self.csend, self.crecv) = refs

    def mate(self, k):
        return self.team * GROUP + lax.rem(self.seat + k, GROUP)

    def peer(self, k):
        return lax.rem(self.team + k, self.groups) * GROUP + self.seat

    def copy(self, src, dst, send, recv, device):
        return pltpu.make_async_remote_copy(
            src_ref=src, dst_ref=dst, send_sem=send, recv_sem=recv,
            device_id=(device,), device_id_type=MESH,
        )

    def ahead(self, k):
        to = lax.rem(self.seat + k, GROUP)
        return self.copy(
            self.mine.at[to], self.got.at[k], self.asend.at[k], self.arecv.at[k], self.mate(k)
        )

    def across(self, k):
        return self.copy(
            self.part, self.gotb.at[k], self.bsend.at[k], self.brecv.at[k], self.peer(k)
        )

    def back(self, k):
        own = self.gathered.at[self.seat]
        return self.copy(own, own, self.csend.at[k], self.crecv.at[k], self.mate(k))

    def scatter(self, value):
        self.mine[...] = value.reshape(self.mine.shape)
        for k in range(1, GROUP):
            self.ahead(k).start()

    def middle(self):
        summed = self.mine[self.seat]
        for k in range(1, GROUP):
            self.ahead(k).wait_recv()
            summed = summed + self.got[k]
        self.part[...] = summed

        def start(k, _):
            self.across(k).start()
            return 0

        lax.fori_loop(1, self.groups, start, 0)

    def post(self):
        def arrive(k, value):
            self.across(k).wait_recv()
            return value + self.gotb[k]

        self.gathered[self.seat] = lax.fori_loop(1, self.groups, arrive, self.part[...])
        for k in range(1, GROUP):
            self.back(k).start()

    def finish(self):
        for k in range(1, GROUP):
            self.back(k).wait_recv()
        value = self.gathered[...].reshape(GROUP * self.part.shape[0], LANE)
        for k in range(1, GROUP):
            self.ahead(k).wait_send()
            self.back(k).wait_send()

        def sent(k, _):
            self.across(k).wait_send()
            return 0

        lax.fori_loop(1, self.groups, sent, 0)
        return value

    @staticmethod
    def scratch(n, rows):
        groups, share = n // GROUP, rows // GROUP
        vm, dma = pltpu.VMEM, pltpu.SemaphoreType.DMA
        return [
            vm((GROUP, share, LANE), F32), vm((GROUP, share, LANE), F32),
            vm((share, LANE), F32), vm((groups, share, LANE), F32),
            vm((GROUP, share, LANE), F32),
            dma((GROUP,)), dma((GROUP,)), dma((groups,)), dma((groups,)),
            dma((GROUP,)), dma((GROUP,)),
        ]


def main_kernel(
    n, total, source, band, offsets, *rest
):
    pieces = source.shape[1] // PIECE
    packs, (once, gram) = rest[:pieces], rest[pieces : pieces + 2]
    (z0, z1, z2, z3, sv, bv, ov, ls, hs, lb, hb, bands,
     local_sem, hsend, hrecv, *totals) = rest[pieces + 2 :]
    me = lax.axis_index("rows")
    right, left = lax.rem(me + 1, n), lax.rem(me + n - 1, n)
    near = Total(n, totals[: len(totals) // 2])
    far = Total(n, totals[len(totals) // 2 :])
    local = source.shape[1]
    blocks = local // HB
    deep_s, deep_b = 3 * HB, 2 * HB
    barrier = pltpu.get_barrier_semaphore()

    def greet(device):
        pl.semaphore_signal(barrier, inc=1, device_id=(device,), device_id_type=MESH)

    def greet_peer(k, _):
        greet(near.peer(k))
        return 0

    greet(left)
    greet(right)
    lax.fori_loop(1, near.groups, greet_peer, 0)
    for k in range(1, GROUP):
        greet(near.mate(k))
    whole = pl.ds(0, offsets.shape[1])
    half = local // 2
    cuts = [
        (source, sv, pl.ds(0, deep_s)), (source, sv, pl.ds(local - deep_s, deep_s)),
        (source, sv, pl.ds(deep_s, local - 2 * deep_s)),
        (offsets, ov, whole),
        (band, bv, pl.ds(0, half)), (band, bv, pl.ds(half, half)),
    ]
    loads = [
        pltpu.make_async_copy(src.at[:, where], dst.at[:, where], local_sem.at[index])
        for index, (src, dst, where) in enumerate(cuts)
    ]
    for load in loads:
        load.start()
    for load in loads[:4]:
        load.wait()
    diagonals = band.shape[0]
    places = lax.broadcasted_iota(jnp.int32, (3 * HB, diagonals), 0)
    chosen = jnp.where(places == ov[...] + HB, 1.0, 0.0).T.astype(BF16)
    chosen = jnp.concatenate([chosen, chosen], axis=0)

    def turn(at, _):
        z0[block(at + 3)] = pack_columns(sv[:, block(at)])
        return 0

    lax.fori_loop(0, blocks, turn, 0, unroll=blocks // 2)

    def build(at, _):
        bands[at + 2] = band_block(bv[:, block(at)], chosen)
        return 0

    loads[4].wait()
    lax.fori_loop(0, blocks // 2, build, 0, unroll=blocks // 2)
    loads[5].wait()
    pl.semaphore_wait(barrier, 2 + GROUP - 1 + near.groups - 1)
    near_low, near_high = pl.ds(0, HB), pl.ds(local - HB, HB)
    far_low, far_high = pl.ds(HB, deep_b), pl.ds(local - deep_s, deep_b)
    own_low, own_high = pl.ds(0, deep_b), pl.ds(local - deep_b, deep_b)
    last, first = pl.ds(deep_b, HB), pl.ds(0, HB)
    moves = (
        (sv.at[:, near_high], ls.at[:, last], right),
        (sv.at[:, near_low], hs.at[:, first], left),
        (sv.at[:, far_high], ls.at[:, own_low], right),
        (sv.at[:, far_low], hs.at[:, far_low], left),
        (bv.at[:, own_high], lb, right),
        (bv.at[:, own_low], hb, left),
    )
    halo = [
        near.copy(src, dst, hsend.at[index], hrecv.at[index], target)
        for index, (src, dst, target) in enumerate(moves)
    ]
    for copy in halo:
        copy.start()
    lax.fori_loop(blocks // 2, blocks, build, 0, unroll=blocks // 2)
    apply_band(bands, 0, z0, z1, True, 3, blocks - 2)

    def edge_source(k):
        part_low = jnp.where(me > 0, ls[:, pl.ds(k * HB, HB)], 0.0)
        z0[pl.ds(k * HB, HB)] = pack_columns(part_low)
        k = 2 - k
        part_high = jnp.where(me < n - 1, hs[:, pl.ds(k * HB, HB)], 0.0)
        z0[pl.ds(3 * HB + local + k * HB, HB)] = pack_columns(part_high)

    for copy in halo[:2]:
        copy.wait_recv()
    edge_source(2)
    apply_band(bands, 0, z0, z1, True, 2, 1)
    apply_band(bands, 0, z0, z1, True, blocks + 1, 1)
    high, low = mixed(z0[pl.ds(3 * HB, local)], z1[pl.ds(2 * HB, local)])
    product = bf(high, jnp.concatenate([high, low], axis=1), TN)
    cross = swap(product[:, LANE:])
    near.scatter(product[:, :LANE] + cross + cross.T)

    for copy in halo[2:]:
        copy.wait_recv()
    for k in range(2):
        edge_source(k)
        part_low = jnp.where(me > 0, lb[:, pl.ds(k * HB, HB)], 0.0)
        part_high = jnp.where(me < n - 1, hb[:, pl.ds(k * HB, HB)], 0.0)
        bands[k] = band_block(part_low, chosen)
        bands[2 + blocks + k] = band_block(part_high, chosen)
    apply_band(bands, 0, z0, z1, True, 0, 2)
    apply_band(bands, 0, z0, z1, True, blocks + 2, 2)
    apply_band(bands, 1, z1, z2, False, 0, blocks + 2)
    near.middle()
    apply_band(bands, 2, z2, z3, True, 0, blocks)
    high, low = mixed(z0[pl.ds(3 * HB, local)], z1[pl.ds(2 * HB, local)])
    high2, low2 = mixed(z2[pl.ds(HB, local)], z3[...])
    product = bf(high2, jnp.concatenate([high, low, high2, low2], axis=1), TN)
    other = bf(high, low2, TN)
    cross = (product[:, :LANE] + swap(product[:, LANE : 2 * LANE])).T + swap(other)
    own = swap(product[:, 3 * LANE :])
    own = product[:, 2 * LANE : 3 * LANE] + own + own.T
    far.scatter(jnp.concatenate([cross, own], axis=0))
    for index, out in enumerate(packs):
        for at, z in enumerate((z0, z1, z2, z3)):
            where = pl.ds(index * PIECE + (3 - at) * HB, PIECE)
            out[:, at * LANE : (at + 1) * LANE] = z[where]
    near.post()
    far.middle()
    gram_one = near.finish() * (1.0 / total)
    turned = square_turn(gram_one, gram_one)
    far.post()
    once[...] = square_turn(exact(turned, gram_one), gram_one)
    gram[...] = far.finish() * (1.0 / total)
    for copy in halo:
        copy.wait_send()


def make_main(source, band, offsets, total):
    n = lax.axis_size("rows")
    width, local = source.shape
    diagonals = band.shape[0]
    blocks = local // HB
    dma = pltpu.SemaphoreType.DMA
    shape = jax.ShapeDtypeStruct
    vm = pltpu.VMEM
    return pl.pallas_call(
        functools.partial(main_kernel, n, total),
        out_shape=[
            shape((PIECE, 4 * LANE), BF16) for _ in range(local // PIECE)
        ]
        + [shape((LANE, LANE), F32), shape((2 * LANE, LANE), F32)],
        in_specs=[HBM] * 3,
        out_specs=[VMEM] * (local // PIECE + 2),
        scratch_shapes=[
            vm((local + 6 * HB, LANE), BF16),
            vm((local + 4 * HB, LANE), BF16),
            vm((local + 2 * HB, LANE), BF16),
            vm((local, LANE), BF16),
            vm((width, local), F32),
            vm((diagonals, local), F32),
            vm((1, diagonals), jnp.int32),
            vm((width, 3 * HB), F32), vm((width, 3 * HB), F32),
            vm((diagonals, 2 * HB), F32), vm((diagonals, 2 * HB), F32),
            vm((blocks + 4, HB, 6 * HB), BF16),
            dma((6,)), dma((6,)), dma((6,)),
        ]
        + Total.scratch(n, LANE)
        + Total.scratch(n, 2 * LANE),
        compiler_params=pltpu.CompilerParams(
            collective_id=0, has_side_effects=True, vmem_limit_bytes=49 << 20
        ),
    )(source, band, offsets.reshape(1, diagonals))


def splat(value):
    return jnp.broadcast_to(value, (SUB, LANE))


def eliminate(metric, right):
    tiles = metric.shape[0] // SUB
    part = [slice(SUB * t, SUB * t + SUB) for t in range(tiles)]
    state = [[metric[part[t]], right[part[t]]] for t in range(tiles)]
    rows = lax.broadcasted_iota(jnp.int32, (SUB, LANE), 0)
    solved = []
    steps = range(SUB)
    for t0 in range(tiles):
        at = SUB * t0
        core = {
            (i, k): splat(state[t0][0][i : i + 1, at + k : at + k + 1])
            for i in steps
            for k in range(i, SUB)
        }
        pivots = [[splat(half[i : i + 1]) for half in state[t0]] for i in steps]
        inverse = []
        for i in steps:
            inverse.append(1.0 / core[i, i])
            for k in range(i + 1, SUB):
                ratio = core[i, k] * inverse[i]
                for m in range(k, SUB):
                    core[k, m] = core[k, m] - ratio * core[i, m]
                pivots[k] = [p - ratio * q for p, q in zip(pivots[k], pivots[i])]
        result = jnp.zeros((SUB, LANE), F32)
        for i in steps:
            result = jnp.where(rows == i, pivots[i][1] * lax.rsqrt(core[i, i]), result)
        solved.append(result)
        for t in range(t0 + 1, tiles):
            scaled = []
            for k in steps:
                column = splat(state[t][0][:, at + k : at + k + 1])
                for i in range(k):
                    column = column - scaled[i] * core[i, k]
                scaled.append(column * inverse[k])
            for half in range(2):
                value = state[t][half]
                for k in steps:
                    value = value - scaled[k] * pivots[k][half]
                state[t][half] = value
    return jnp.concatenate(solved, axis=0)


def square_turn(spanning, grammian):
    return eliminate(exact(exact(spanning, grammian), spanning, NT), spanning)


def last_kernel(once, gram, *rest):
    *packs, out, tile, sem = rest
    keep = LANE
    coeffs = once[...]
    cross, far = gram[:keep], gram[keep:]
    cross = exact(exact(coeffs, cross), coeffs, NT)
    far = exact(exact(coeffs, far), coeffs, NT)
    across = lax.broadcasted_iota(jnp.int32, (keep, keep), 1)
    down = lax.broadcasted_iota(jnp.int32, (keep, keep), 0)
    unit = jnp.where(across == down, 1.0, 0.0)
    span_a = unit + exact(cross, cross, NT)
    span_b = cross + exact(cross, far)
    next_a = span_a + exact(span_b, cross, NT)
    next_b = exact(span_a, cross) + exact(span_b, far)
    metric = exact(next_a, span_a, NT) + exact(next_b, span_b, NT)
    spanning = jnp.concatenate([exact(span_a, coeffs), exact(span_b, coeffs)], axis=1)
    coeffs = exact(eliminate(metric, unit), spanning)
    turned = coeffs.T
    half = LANE // 2
    weights = jnp.concatenate(halves(turned), axis=1)
    weights = jnp.concatenate(
        [weights[half * (k // 2) : half * (k // 2) + half] for k in range(8)], axis=0
    )
    stores = []
    for at, piece in enumerate(packs):
        both = bf(piece[...], weights)
        tile[at] = (both[:, :LANE] + both[:, LANE:]).T
        stores.append(
            pltpu.make_async_copy(
                tile.at[at], out.at[:, pl.ds(at * PIECE, PIECE)], sem.at[at]
            )
        )
        stores[-1].start()
    for store in stores:
        store.wait()


def make_last(packs, once, gram):
    count = len(packs)
    return pl.pallas_call(
        last_kernel,
        out_shape=jax.ShapeDtypeStruct((LANE, count * PIECE), F32),
        in_specs=[VMEM] * (count + 2),
        out_specs=HBM,
        scratch_shapes=[
            pltpu.VMEM((count, LANE, PIECE), F32),
            pltpu.SemaphoreType.DMA((count,)),
        ],
        compiler_params=pltpu.CompilerParams(vmem_limit_bytes=28 << 20),
    )(once, gram, *packs)


def body(source, band_values, offsets):
    total = float(source.shape[1] * lax.axis_size("rows"))
    *packs, once, gram = make_main(source, band_values, offsets, total)
    return make_last(packs, once, gram)


def solution(mesh):
    placed = (P(None, "rows"), P(None, "rows"), P())
    return jax.shard_map(
        body, mesh=mesh, in_specs=placed, out_specs=P(None, "rows"), check_vma=False
    )
```

```python
import functools

import jax
import jax.numpy as jnp
from jax import lax
from jax.experimental import pallas as pl
from jax.experimental.pallas import tpu as pltpu
from jax.sharding import PartitionSpec as P

HB = 128
SUB = 8
LANE = 128
GROUP = 8
PANEL = 4
PIECE = 4 * HB
MESH = pl.DeviceIdType.MESH
VMEM = pl.BlockSpec(memory_space=pltpu.VMEM)
HBM = pl.BlockSpec(memory_space=pltpu.HBM)
NN = (((1,), (0,)), ((), ()))
NT = (((1,), (1,)), ((), ()))
TN = (((0,), (0,)), ((), ()))
F32 = jnp.float32
BF16 = jnp.bfloat16


def bf(a, b, dims=NN):
    return lax.dot_general(a, b, dims, preferred_element_type=F32)


def thirds(value):
    top = value.astype(BF16)
    rest = value - top.astype(F32)
    middle = rest.astype(BF16)
    return top, middle, (rest - middle.astype(F32)).astype(BF16)


def exact(a, b, dims=NN):
    (at,), (bt,) = dims[0]
    a1, a2, a3 = thirds(a)
    b1, b2, b3 = thirds(b)
    left = jnp.concatenate([a1, a1, a2, a2, a1, a3], axis=at)
    return bf(left, jnp.concatenate([b1, b2, b1, b2, b3, b1], axis=bt), dims)


def halves(value):
    high = value.astype(BF16)
    low = (value - high.astype(F32)).astype(BF16)
    return high, low


def block(at, count=1):
    return pl.ds(pl.multiple_of(at * HB, HB), count * HB)


def pack(twice, flip):
    lanes = lax.broadcasted_iota(jnp.int32, twice.shape, 1)
    high = twice.astype(BF16).astype(F32)
    return jnp.where((lanes < LANE // 2) != flip, high, twice - high).astype(BF16)


def pack_columns(part):
    return pack(jnp.concatenate([part, part], axis=0).T, False)


def band_block(values, chosen):
    top, bottom = halves(values.T)
    spread = bf(jnp.concatenate([top, bottom], axis=1), chosen)
    sheared = pltpu.roll(spread, 0, 1, stride=1, stride_axis=0)
    return jnp.concatenate(halves(sheared), axis=1)


def apply_band(bands, skip, z, out, flip, start, count):
    def step(k, _):
        at = start + k
        window = z[block(at, 3)]
        both = bf(bands[at + skip], jnp.concatenate([window, window], axis=0))
        out[block(at)] = pack(both + pltpu.roll(both, LANE // 2, 1), flip)
        return 0

    lax.fori_loop(0, count, step, 0, unroll=count)


def swap(value):
    return pltpu.roll(value, LANE // 2, 1)


def mixed(even, odd):
    lanes = lax.broadcasted_iota(jnp.int32, even.shape, 1)
    first = lanes < LANE // 2
    return jnp.where(first, even, odd), jnp.where(first, odd, even)


class Total:
    def __init__(self, n, refs):
        self.groups = n // GROUP
        me = lax.axis_index("rows")
        self.team, self.seat = me // GROUP, lax.rem(me, GROUP)
        (self.mine, self.got, self.part, self.gotb, self.gathered,
         self.asend, self.arecv, self.bsend, self.brecv, self.csend, self.crecv) = refs

    def mate(self, k):
        return self.team * GROUP + lax.rem(self.seat + k, GROUP)

    def peer(self, k):
        return lax.rem(self.team + k, self.groups) * GROUP + self.seat

    def copy(self, src, dst, send, recv, device):
        return pltpu.make_async_remote_copy(
            src_ref=src, dst_ref=dst, send_sem=send, recv_sem=recv,
            device_id=(device,), device_id_type=MESH,
        )

    def ahead(self, k):
        to = lax.rem(self.seat + k, GROUP)
        return self.copy(
            self.mine.at[to], self.got.at[k], self.asend.at[k], self.arecv.at[k], self.mate(k)
        )

    def across(self, k):
        return self.copy(
            self.part, self.gotb.at[k], self.bsend.at[k], self.brecv.at[k], self.peer(k)
        )

    def back(self, k):
        own = self.gathered.at[self.seat]
        return self.copy(own, own, self.csend.at[k], self.crecv.at[k], self.mate(k))

    def scatter(self, value):
        self.mine[...] = value.reshape(self.mine.shape)
        for k in range(1, GROUP):
            self.ahead(k).start()

    def middle(self):
        summed = self.mine[self.seat]
        for k in range(1, GROUP):
            self.ahead(k).wait_recv()
            summed = summed + self.got[k]
        self.part[...] = summed

        def start(k, _):
            self.across(k).start()
            return 0

        lax.fori_loop(1, self.groups, start, 0)

    def post(self):
        def arrive(k, value):
            self.across(k).wait_recv()
            return value + self.gotb[k]

        self.gathered[self.seat] = lax.fori_loop(1, self.groups, arrive, self.part[...])
        for k in range(1, GROUP):
            self.back(k).start()

    def finish(self):
        for k in range(1, GROUP):
            self.back(k).wait_recv()
        value = self.gathered[...].reshape(GROUP * self.part.shape[0], LANE)
        for k in range(1, GROUP):
            self.ahead(k).wait_send()
            self.back(k).wait_send()

        def sent(k, _):
            self.across(k).wait_send()
            return 0

        lax.fori_loop(1, self.groups, sent, 0)
        return value

    @staticmethod
    def scratch(n, rows):
        groups, share = n // GROUP, rows // GROUP
        vm, dma = pltpu.VMEM, pltpu.SemaphoreType.DMA
        return [
            vm((GROUP, share, LANE), F32), vm((GROUP, share, LANE), F32),
            vm((share, LANE), F32), vm((groups, share, LANE), F32),
            vm((GROUP, share, LANE), F32),
            dma((GROUP,)), dma((GROUP,)), dma((groups,)), dma((groups,)),
            dma((GROUP,)), dma((GROUP,)),
        ]


def main_kernel(
    n, total, source, band, offsets, *rest
):
    pieces = source.shape[1] // PIECE
    packs, (once, gram) = rest[:pieces], rest[pieces : pieces + 2]
    (z0, z1, z2, z3, sv, bv, ov, ls, hs, lb, hb, bands,
     local_sem, hsend, hrecv, *totals) = rest[pieces + 2 :]
    me = lax.axis_index("rows")
    right, left = lax.rem(me + 1, n), lax.rem(me + n - 1, n)
    near = Total(n, totals[: len(totals) // 2])
    far = Total(n, totals[len(totals) // 2 :])
    local = source.shape[1]
    blocks = local // HB
    deep_s, deep_b = 3 * HB, 2 * HB
    barrier = pltpu.get_barrier_semaphore()

    def greet(device):
        pl.semaphore_signal(barrier, inc=1, device_id=(device,), device_id_type=MESH)

    def greet_peer(k, _):
        greet(near.peer(k))
        return 0

    greet(left)
    greet(right)
    lax.fori_loop(1, near.groups, greet_peer, 0)
    for k in range(1, GROUP):
        greet(near.mate(k))
    whole = pl.ds(0, offsets.shape[1])
    half = local // 2
    cuts = [
        (source, sv, pl.ds(0, deep_s)), (source, sv, pl.ds(local - deep_s, deep_s)),
        (source, sv, pl.ds(deep_s, local - 2 * deep_s)),
        (offsets, ov, whole),
        (band, bv, pl.ds(0, half)), (band, bv, pl.ds(half, half)),
    ]
    loads = [
        pltpu.make_async_copy(src.at[:, where], dst.at[:, where], local_sem.at[index])
        for index, (src, dst, where) in enumerate(cuts)
    ]
    for load in loads:
        load.start()
    for load in loads[:4]:
        load.wait()
    diagonals = band.shape[0]
    places = lax.broadcasted_iota(jnp.int32, (3 * HB, diagonals), 0)
    chosen = jnp.where(places == ov[...] + HB, 1.0, 0.0).T.astype(BF16)
    chosen = jnp.concatenate([chosen, chosen], axis=0)

    def turn(at, _):
        z0[block(at + 3)] = pack_columns(sv[:, block(at)])
        return 0

    lax.fori_loop(0, blocks, turn, 0, unroll=blocks // 2)

    def build(at, _):
        bands[at + 2] = band_block(bv[:, block(at)], chosen)
        return 0

    pl.semaphore_wait(barrier, 2 + GROUP - 1 + near.groups - 1)
    near_low, near_high = pl.ds(0, HB), pl.ds(local - HB, HB)
    far_low, far_high = pl.ds(HB, deep_b), pl.ds(local - deep_s, deep_b)
    own_low, own_high = pl.ds(0, deep_b), pl.ds(local - deep_b, deep_b)
    last, first = pl.ds(deep_b, HB), pl.ds(0, HB)
    moves = (
        (sv.at[:, near_high], ls.at[:, last], right),
        (sv.at[:, near_low], hs.at[:, first], left),
        (sv.at[:, far_high], ls.at[:, own_low], right),
        (sv.at[:, far_low], hs.at[:, far_low], left),
        (bv.at[:, own_high], lb, right),
        (bv.at[:, own_low], hb, left),
    )
    halo = [
        near.copy(src, dst, hsend.at[index], hrecv.at[index], target)
        for index, (src, dst, target) in enumerate(moves)
    ]
    for copy in halo[:4]:
        copy.start()
    loads[4].wait()
    loads[5].wait()
    for copy in halo[4:]:
        copy.start()
    lax.fori_loop(0, blocks, build, 0, unroll=blocks)
    apply_band(bands, 0, z0, z1, True, 3, blocks - 2)

    def edge_source(k):
        part_low = jnp.where(me > 0, ls[:, pl.ds(k * HB, HB)], 0.0)
        z0[pl.ds(k * HB, HB)] = pack_columns(part_low)
        k = 2 - k
        part_high = jnp.where(me < n - 1, hs[:, pl.ds(k * HB, HB)], 0.0)
        z0[pl.ds(3 * HB + local + k * HB, HB)] = pack_columns(part_high)

    for copy in halo[:2]:
        copy.wait_recv()
    edge_source(2)
    apply_band(bands, 0, z0, z1, True, 2, 1)
    apply_band(bands, 0, z0, z1, True, blocks + 1, 1)
    high, low = mixed(z0[pl.ds(3 * HB, local)], z1[pl.ds(2 * HB, local)])
    product = bf(high, jnp.concatenate([high, low], axis=1), TN)
    cross = swap(product[:, LANE:])
    near.scatter(product[:, :LANE] + cross + cross.T)

    for copy in halo[2:]:
        copy.wait_recv()
    for k in range(2):
        edge_source(k)
        part_low = jnp.where(me > 0, lb[:, pl.ds(k * HB, HB)], 0.0)
        part_high = jnp.where(me < n - 1, hb[:, pl.ds(k * HB, HB)], 0.0)
        bands[k] = band_block(part_low, chosen)
        bands[2 + blocks + k] = band_block(part_high, chosen)
    apply_band(bands, 0, z0, z1, True, 0, 2)
    apply_band(bands, 0, z0, z1, True, blocks + 2, 2)
    apply_band(bands, 1, z1, z2, False, 0, blocks + 2)
    near.middle()
    apply_band(bands, 2, z2, z3, True, 0, blocks)
    high, low = mixed(z0[pl.ds(3 * HB, local)], z1[pl.ds(2 * HB, local)])
    high2, low2 = mixed(z2[pl.ds(HB, local)], z3[...])
    product = bf(high2, jnp.concatenate([high, low, high2, low2], axis=1), TN)
    other = bf(high, low2, TN)
    cross = (product[:, :LANE] + swap(product[:, LANE : 2 * LANE])).T + swap(other)
    own = swap(product[:, 3 * LANE :])
    own = product[:, 2 * LANE : 3 * LANE] + own + own.T
    far.scatter(jnp.concatenate([cross, own], axis=0))
    for index, out in enumerate(packs):
        for at, z in enumerate((z0, z1, z2, z3)):
            where = pl.ds(index * PIECE + (3 - at) * HB, PIECE)
            out[:, at * LANE : (at + 1) * LANE] = z[where]
    near.post()
    far.middle()
    gram_one = near.finish() * (1.0 / total)
    turned = square_turn(gram_one, gram_one)
    far.post()
    once[...] = square_turn(exact(turned, gram_one), gram_one)
    gram[...] = far.finish() * (1.0 / total)
    for copy in halo:
        copy.wait_send()


def make_main(source, band, offsets, total):
    n = lax.axis_size("rows")
    width, local = source.shape
    diagonals = band.shape[0]
    blocks = local // HB
    dma = pltpu.SemaphoreType.DMA
    shape = jax.ShapeDtypeStruct
    vm = pltpu.VMEM
    return pl.pallas_call(
        functools.partial(main_kernel, n, total),
        out_shape=[
            shape((PIECE, 4 * LANE), BF16) for _ in range(local // PIECE)
        ]
        + [shape((LANE, LANE), F32), shape((2 * LANE, LANE), F32)],
        in_specs=[HBM] * 3,
        out_specs=[VMEM] * (local // PIECE + 2),
        scratch_shapes=[
            vm((local + 6 * HB, LANE), BF16),
            vm((local + 4 * HB, LANE), BF16),
            vm((local + 2 * HB, LANE), BF16),
            vm((local, LANE), BF16),
            vm((width, local), F32),
            vm((diagonals, local), F32),
            vm((1, diagonals), jnp.int32),
            vm((width, 3 * HB), F32), vm((width, 3 * HB), F32),
            vm((diagonals, 2 * HB), F32), vm((diagonals, 2 * HB), F32),
            vm((blocks + 4, HB, 6 * HB), BF16),
            dma((6,)), dma((6,)), dma((6,)),
        ]
        + Total.scratch(n, LANE)
        + Total.scratch(n, 2 * LANE),
        compiler_params=pltpu.CompilerParams(
            collective_id=0, has_side_effects=True, vmem_limit_bytes=49 << 20
        ),
    )(source, band, offsets.reshape(1, diagonals))


def splat(value):
    return jnp.broadcast_to(value, (SUB, LANE))


def outer(rows):
    a, b, c = thirds(rows)
    left = jnp.concatenate([part[:, :LANE] for part in (a, a, b, b, a, c)], axis=0)
    return bf(left, jnp.concatenate([a, b, a, b, c, a], axis=0), TN)


def column(value, k):
    return splat(value[:, k : k + 1])


def eliminate(metric, right):
    tiles = metric.shape[0] // SUB
    state = [
        [metric[SUB * t : SUB * t + SUB], right[SUB * t : SUB * t + SUB]] for t in range(tiles)
    ]
    rows = lax.broadcasted_iota(jnp.int32, (SUB, LANE), 0)
    steps = range(SUB)
    columns = [column(state[0][0], k) for k in steps]
    done = []
    for t0 in range(tiles):
        at = SUB * t0
        if t0 + 1 < tiles:
            ahead = state[t0 + 1][0]
            raw = [column(ahead, at + k) for k in steps]
            following = [column(ahead, at + SUB + k) for k in steps]
        core, inverse, pivots = {}, [], []
        roots = jnp.ones((SUB, LANE), F32)
        for i in steps:
            for k in range(i, SUB):
                core[i, k] = splat(columns[k][i : i + 1])
            inverse.append(1.0 / core[i, i])
            roots = jnp.where(rows == i, lax.rsqrt(core[i, i]), roots)
            pivots.append([splat(half[i : i + 1]) for half in state[t0]])
            if i < SUB - 1:
                below = jnp.where(rows > i, columns[i], 0.0)
                for k in range(i + 1, SUB):
                    columns[k] = columns[k] - (below * core[i, k]) * inverse[i]
                ratio = below * inverse[i]
                state[t0] = [half - ratio * p for half, p in zip(state[t0], pivots[i])]
        done.append([half * roots for half in state[t0]])
        limit = min(tiles, PANEL * (t0 // PANEL + 2))
        for t in range(t0 + 1, limit):
            plain, scaled = [], []
            for k in steps:
                value = raw[k] if t == t0 + 1 else column(state[t][0], at + k)
                for i in range(k):
                    value = value - scaled[i] * core[i, k]
                plain.append(value)
                scaled.append(value * inverse[k])
            if t == t0 + 1:
                columns = []
                for j in steps:
                    value = following[j]
                    for k in steps:
                        value = value - scaled[k] * splat(plain[k][j : j + 1])
                    columns.append(value)
            for half in range(2):
                value = state[t][half]
                for k in steps:
                    value = value - scaled[k] * pivots[k][half]
                state[t][half] = value
        if (t0 + 1) % PANEL == 0 and limit < tiles:
            panel = [jnp.concatenate(tile, axis=1) for tile in done[-PANEL:]]
            update = outer(jnp.concatenate(panel, axis=0))
            for t in range(limit, tiles):
                cut = update[SUB * t : SUB * t + SUB]
                state[t] = [state[t][0] - cut[:, :LANE], state[t][1] - cut[:, LANE:]]
    return jnp.concatenate([tile[1] for tile in done], axis=0)


def square_turn(spanning, grammian):
    return eliminate(exact(exact(spanning, grammian), spanning, NT), spanning)


def last_kernel(once, gram, *rest):
    *packs, out, tile, sem = rest
    keep = LANE
    coeffs = once[...]
    cross, far = gram[:keep], gram[keep:]
    cross = exact(exact(coeffs, cross), coeffs, NT)
    far = exact(exact(coeffs, far), coeffs, NT)
    across = lax.broadcasted_iota(jnp.int32, (keep, keep), 1)
    down = lax.broadcasted_iota(jnp.int32, (keep, keep), 0)
    unit = jnp.where(across == down, 1.0, 0.0)
    span_a = unit + exact(cross, cross, NT)
    span_b = cross + exact(cross, far)
    next_a = span_a + exact(span_b, cross, NT)
    next_b = exact(span_a, cross) + exact(span_b, far)
    metric = exact(next_a, span_a, NT) + exact(next_b, span_b, NT)
    spanning = jnp.concatenate([exact(span_a, coeffs), exact(span_b, coeffs)], axis=1)
    coeffs = exact(eliminate(metric, unit), spanning)
    turned = coeffs.T
    half = LANE // 2
    weights = jnp.concatenate(halves(turned), axis=1)
    weights = jnp.concatenate(
        [weights[half * (k // 2) : half * (k // 2) + half] for k in range(8)], axis=0
    )
    stores = []
    for at, piece in enumerate(packs):
        both = bf(piece[...], weights)
        tile[at] = (both[:, :LANE] + both[:, LANE:]).T
        stores.append(
            pltpu.make_async_copy(
                tile.at[at], out.at[:, pl.ds(at * PIECE, PIECE)], sem.at[at]
            )
        )
        stores[-1].start()
    for store in stores:
        store.wait()


def make_last(packs, once, gram):
    count = len(packs)
    return pl.pallas_call(
        last_kernel,
        out_shape=jax.ShapeDtypeStruct((LANE, count * PIECE), F32),
        in_specs=[VMEM] * (count + 2),
        out_specs=HBM,
        scratch_shapes=[
            pltpu.VMEM((count, LANE, PIECE), F32),
            pltpu.SemaphoreType.DMA((count,)),
        ],
        compiler_params=pltpu.CompilerParams(vmem_limit_bytes=28 << 20),
    )(once, gram, *packs)


def body(source, band_values, offsets):
    total = float(source.shape[1] * lax.axis_size("rows"))
    *packs, once, gram = make_main(source, band_values, offsets, total)
    return make_last(packs, once, gram)


def solution(mesh):
    placed = (P(None, "rows"), P(None, "rows"), P())
    return jax.shard_map(
        body, mesh=mesh, in_specs=placed, out_specs=P(None, "rows"), check_vma=False
    )
```

```python
import functools

import jax
import jax.numpy as jnp
from jax import lax
from jax.experimental import pallas as pl
from jax.experimental.pallas import tpu as pltpu
from jax.sharding import PartitionSpec as P

HB = 128
SUB = 8
LANE = 128
GROUP = 8
PANEL = 4
PIECE = 4 * HB
MESH = pl.DeviceIdType.MESH
VMEM = pl.BlockSpec(memory_space=pltpu.VMEM)
HBM = pl.BlockSpec(memory_space=pltpu.HBM)
NN = (((1,), (0,)), ((), ()))
NT = (((1,), (1,)), ((), ()))
TN = (((0,), (0,)), ((), ()))
F32 = jnp.float32
BF16 = jnp.bfloat16


def bf(a, b, dims=NN):
    return lax.dot_general(a, b, dims, preferred_element_type=F32)


def thirds(value):
    top = value.astype(BF16)
    rest = value - top.astype(F32)
    middle = rest.astype(BF16)
    return top, middle, (rest - middle.astype(F32)).astype(BF16)


def exact(a, b, dims=NN):
    (at,), (bt,) = dims[0]
    a1, a2, a3 = thirds(a)
    b1, b2, b3 = thirds(b)
    left = jnp.concatenate([a1, a1, a2, a2, a1, a3], axis=at)
    return bf(left, jnp.concatenate([b1, b2, b1, b2, b3, b1], axis=bt), dims)


def halves(value):
    high = value.astype(BF16)
    low = (value - high.astype(F32)).astype(BF16)
    return high, low


def block(at, count=1):
    return pl.ds(pl.multiple_of(at * HB, HB), count * HB)


def pack(twice, flip):
    lanes = lax.broadcasted_iota(jnp.int32, twice.shape, 1)
    high = twice.astype(BF16).astype(F32)
    return jnp.where((lanes < LANE // 2) != flip, high, twice - high).astype(BF16)


def pack_columns(part):
    return pack(jnp.concatenate([part, part], axis=0).T, False)


def band_block(values, chosen):
    top, bottom = halves(values.T)
    spread = bf(jnp.concatenate([top, bottom], axis=1), chosen)
    sheared = pltpu.roll(spread, 0, 1, stride=1, stride_axis=0)
    return jnp.concatenate(halves(sheared), axis=1)


def apply_band(bands, skip, z, out, flip, start, count):
    def step(k, _):
        at = start + k
        window = z[block(at, 3)]
        both = bf(bands[at + skip], jnp.concatenate([window, window], axis=0))
        out[block(at)] = pack(both + pltpu.roll(both, LANE // 2, 1), flip)
        return 0

    lax.fori_loop(0, count, step, 0, unroll=count)


def swap(value):
    return pltpu.roll(value, LANE // 2, 1)


def mixed(even, odd):
    lanes = lax.broadcasted_iota(jnp.int32, even.shape, 1)
    first = lanes < LANE // 2
    return jnp.where(first, even, odd), jnp.where(first, odd, even)


class Total:
    def __init__(self, n, refs):
        self.groups = n // GROUP
        me = lax.axis_index("rows")
        self.team, self.seat = me // GROUP, lax.rem(me, GROUP)
        (self.mine, self.got, self.part, self.gotb, self.gathered,
         self.asend, self.arecv, self.bsend, self.brecv, self.csend, self.crecv) = refs

    def mate(self, k):
        return self.team * GROUP + lax.rem(self.seat + k, GROUP)

    def peer(self, k):
        return lax.rem(self.team + k, self.groups) * GROUP + self.seat

    def copy(self, src, dst, send, recv, device):
        return pltpu.make_async_remote_copy(
            src_ref=src, dst_ref=dst, send_sem=send, recv_sem=recv,
            device_id=(device,), device_id_type=MESH,
        )

    def ahead(self, k):
        to = lax.rem(self.seat + k, GROUP)
        return self.copy(
            self.mine.at[to], self.got.at[k], self.asend.at[k], self.arecv.at[k], self.mate(k)
        )

    def across(self, k):
        return self.copy(
            self.part, self.gotb.at[k], self.bsend.at[k], self.brecv.at[k], self.peer(k)
        )

    def back(self, k):
        own = self.gathered.at[self.seat]
        return self.copy(own, own, self.csend.at[k], self.crecv.at[k], self.mate(k))

    def scatter(self, value):
        self.mine[...] = value.reshape(self.mine.shape)
        for k in range(1, GROUP):
            self.ahead(k).start()

    def middle(self):
        summed = self.mine[self.seat]
        for k in range(1, GROUP):
            self.ahead(k).wait_recv()
            summed = summed + self.got[k]
        self.part[...] = summed

        def start(k, _):
            self.across(k).start()
            return 0

        lax.fori_loop(1, self.groups, start, 0)

    def post(self):
        def arrive(k, value):
            self.across(k).wait_recv()
            return value + self.gotb[k]

        self.gathered[self.seat] = lax.fori_loop(1, self.groups, arrive, self.part[...])
        for k in range(1, GROUP):
            self.back(k).start()

    def finish(self):
        for k in range(1, GROUP):
            self.back(k).wait_recv()
        value = self.gathered[...].reshape(GROUP * self.part.shape[0], LANE)
        for k in range(1, GROUP):
            self.ahead(k).wait_send()
            self.back(k).wait_send()

        def sent(k, _):
            self.across(k).wait_send()
            return 0

        lax.fori_loop(1, self.groups, sent, 0)
        return value

    @staticmethod
    def scratch(n, rows):
        groups, share = n // GROUP, rows // GROUP
        vm, dma = pltpu.VMEM, pltpu.SemaphoreType.DMA
        return [
            vm((GROUP, share, LANE), F32), vm((GROUP, share, LANE), F32),
            vm((share, LANE), F32), vm((groups, share, LANE), F32),
            vm((GROUP, share, LANE), F32),
            dma((GROUP,)), dma((GROUP,)), dma((groups,)), dma((groups,)),
            dma((GROUP,)), dma((GROUP,)),
        ]


def main_kernel(
    n, total, source, band, offsets, *rest
):
    pieces = source.shape[1] // PIECE
    packs, (once, gram) = rest[:pieces], rest[pieces : pieces + 2]
    (z0, z1, z2, z3, sv, bv, ov, ls, hs, lb, hb, bands,
     local_sem, hsend, hrecv, *totals) = rest[pieces + 2 :]
    me = lax.axis_index("rows")
    right, left = lax.rem(me + 1, n), lax.rem(me + n - 1, n)
    near = Total(n, totals[: len(totals) // 2])
    far = Total(n, totals[len(totals) // 2 :])
    local = source.shape[1]
    blocks = local // HB
    deep_s, deep_b = 3 * HB, 2 * HB
    barrier = pltpu.get_barrier_semaphore()

    def greet(device):
        pl.semaphore_signal(barrier, inc=1, device_id=(device,), device_id_type=MESH)

    def greet_peer(k, _):
        greet(near.peer(k))
        return 0

    greet(left)
    greet(right)
    lax.fori_loop(1, near.groups, greet_peer, 0)
    for k in range(1, GROUP):
        greet(near.mate(k))
    whole = pl.ds(0, offsets.shape[1])
    half = local // 2
    cuts = [
        (source, sv, pl.ds(0, deep_s)), (source, sv, pl.ds(local - deep_s, deep_s)),
        (source, sv, pl.ds(deep_s, local - 2 * deep_s)),
        (offsets, ov, whole),
        (band, bv, pl.ds(0, half)), (band, bv, pl.ds(half, half)),
    ]
    loads = [
        pltpu.make_async_copy(src.at[:, where], dst.at[:, where], local_sem.at[index])
        for index, (src, dst, where) in enumerate(cuts)
    ]
    for load in loads:
        load.start()
    for load in loads[:4]:
        load.wait()
    diagonals = band.shape[0]
    places = lax.broadcasted_iota(jnp.int32, (3 * HB, diagonals), 0)
    chosen = jnp.where(places == ov[...] + HB, 1.0, 0.0).T.astype(BF16)
    chosen = jnp.concatenate([chosen, chosen], axis=0)

    def turn(at, _):
        z0[block(at + 3)] = pack_columns(sv[:, block(at)])
        return 0

    lax.fori_loop(0, blocks, turn, 0, unroll=blocks // 2)

    def build(at, _):
        bands[at + 2] = band_block(bv[:, block(at)], chosen)
        return 0

    pl.semaphore_wait(barrier, 2 + GROUP - 1 + near.groups - 1)
    near_low, near_high = pl.ds(0, HB), pl.ds(local - HB, HB)
    far_low, far_high = pl.ds(HB, deep_b), pl.ds(local - deep_s, deep_b)
    own_low, own_high = pl.ds(0, deep_b), pl.ds(local - deep_b, deep_b)
    last, first = pl.ds(deep_b, HB), pl.ds(0, HB)
    moves = (
        (sv.at[:, near_high], ls.at[:, last], right),
        (sv.at[:, near_low], hs.at[:, first], left),
        (sv.at[:, far_high], ls.at[:, own_low], right),
        (sv.at[:, far_low], hs.at[:, far_low], left),
        (bv.at[:, own_high], lb, right),
        (bv.at[:, own_low], hb, left),
    )
    halo = [
        near.copy(src, dst, hsend.at[index], hrecv.at[index], target)
        for index, (src, dst, target) in enumerate(moves)
    ]
    for copy in halo[:4]:
        copy.start()
    loads[4].wait()
    loads[5].wait()
    for copy in halo[4:]:
        copy.start()
    lax.fori_loop(0, blocks, build, 0, unroll=blocks)
    apply_band(bands, 0, z0, z1, True, 3, blocks - 2)

    def edge_source(k):
        part_low = jnp.where(me > 0, ls[:, pl.ds(k * HB, HB)], 0.0)
        z0[pl.ds(k * HB, HB)] = pack_columns(part_low)
        k = 2 - k
        part_high = jnp.where(me < n - 1, hs[:, pl.ds(k * HB, HB)], 0.0)
        z0[pl.ds(3 * HB + local + k * HB, HB)] = pack_columns(part_high)

    def gram_part(*parts):
        even = jnp.concatenate([z0[pl.ds(at * HB + 3 * HB, size * HB)] for at, size in parts], axis=0)
        odd = jnp.concatenate([z1[pl.ds(at * HB + 2 * HB, size * HB)] for at, size in parts], axis=0)
        high, low = mixed(even, odd)
        return bf(high, jnp.concatenate([high, low], axis=1), TN)

    product = gram_part((1, blocks - 2))
    for copy in halo[:2]:
        copy.wait_recv()
    edge_source(2)
    apply_band(bands, 0, z0, z1, True, 2, 1)
    apply_band(bands, 0, z0, z1, True, blocks + 1, 1)
    product = product + gram_part((0, 1), (blocks - 1, 1))
    cross = swap(product[:, LANE:])
    near.scatter(product[:, :LANE] + cross + cross.T)

    for copy in halo[2:]:
        copy.wait_recv()
    for k in range(2):
        edge_source(k)
        part_low = jnp.where(me > 0, lb[:, pl.ds(k * HB, HB)], 0.0)
        part_high = jnp.where(me < n - 1, hb[:, pl.ds(k * HB, HB)], 0.0)
        bands[k] = band_block(part_low, chosen)
        bands[2 + blocks + k] = band_block(part_high, chosen)
    apply_band(bands, 0, z0, z1, True, 0, 2)
    apply_band(bands, 0, z0, z1, True, blocks + 2, 2)
    apply_band(bands, 1, z1, z2, False, 0, blocks + 2)
    near.middle()
    apply_band(bands, 2, z2, z3, True, 0, blocks)
    high, low = mixed(z0[pl.ds(3 * HB, local)], z1[pl.ds(2 * HB, local)])
    high2, low2 = mixed(z2[pl.ds(HB, local)], z3[...])
    product = bf(high2, jnp.concatenate([high, low, high2, low2], axis=1), TN)
    other = bf(high, low2, TN)
    cross = (product[:, :LANE] + swap(product[:, LANE : 2 * LANE])).T + swap(other)
    own = swap(product[:, 3 * LANE :])
    own = product[:, 2 * LANE : 3 * LANE] + own + own.T
    far.scatter(jnp.concatenate([cross, own], axis=0))
    for index, out in enumerate(packs):
        for at, z in enumerate((z0, z1, z2, z3)):
            where = pl.ds(index * PIECE + (3 - at) * HB, PIECE)
            out[:, at * LANE : (at + 1) * LANE] = z[where]
    near.post()
    far.middle()
    gram_one = near.finish() * (1.0 / total)
    cube = exact(exact(gram_one, gram_one), gram_one)
    turned = eliminate(cube, gram_one)
    far.post()
    spanning = exact(turned, gram_one)
    metric = exact(exact(spanning, gram_one), spanning, NT)
    once[...] = eliminate(metric, spanning)
    gram[...] = far.finish() * (1.0 / total)
    for copy in halo:
        copy.wait_send()


def make_main(source, band, offsets, total):
    n = lax.axis_size("rows")
    width, local = source.shape
    diagonals = band.shape[0]
    blocks = local // HB
    dma = pltpu.SemaphoreType.DMA
    shape = jax.ShapeDtypeStruct
    vm = pltpu.VMEM
    return pl.pallas_call(
        functools.partial(main_kernel, n, total),
        out_shape=[
            shape((PIECE, 4 * LANE), BF16) for _ in range(local // PIECE)
        ]
        + [shape((LANE, LANE), F32), shape((2 * LANE, LANE), F32)],
        in_specs=[HBM] * 3,
        out_specs=[VMEM] * (local // PIECE + 2),
        scratch_shapes=[
            vm((local + 6 * HB, LANE), BF16),
            vm((local + 4 * HB, LANE), BF16),
            vm((local + 2 * HB, LANE), BF16),
            vm((local, LANE), BF16),
            vm((width, local), F32),
            vm((diagonals, local), F32),
            vm((1, diagonals), jnp.int32),
            vm((width, 3 * HB), F32), vm((width, 3 * HB), F32),
            vm((diagonals, 2 * HB), F32), vm((diagonals, 2 * HB), F32),
            vm((blocks + 4, HB, 6 * HB), BF16),
            dma((6,)), dma((6,)), dma((6,)),
        ]
        + Total.scratch(n, LANE)
        + Total.scratch(n, 2 * LANE),
        compiler_params=pltpu.CompilerParams(
            collective_id=0, has_side_effects=True, vmem_limit_bytes=49 << 20
        ),
    )(source, band, offsets.reshape(1, diagonals))


def splat(value):
    return jnp.broadcast_to(value, (SUB, LANE))


def outer(rows):
    a, b, c = thirds(rows)
    left = jnp.concatenate([part[:, :LANE] for part in (a, a, b, b, a, c)], axis=0)
    return bf(left, jnp.concatenate([a, b, a, b, c, a], axis=0), TN)


def column(value, k):
    return splat(value[:, k : k + 1])


def eliminate(metric, right):
    tiles = metric.shape[0] // SUB
    state = [
        [metric[SUB * t : SUB * t + SUB], right[SUB * t : SUB * t + SUB]] for t in range(tiles)
    ]
    rows = lax.broadcasted_iota(jnp.int32, (SUB, LANE), 0)
    steps = range(SUB)
    columns = [column(state[0][0], k) for k in steps]
    done = []
    for t0 in range(tiles):
        at = SUB * t0
        if t0 + 1 < tiles:
            ahead = state[t0 + 1][0]
            raw = [column(ahead, at + k) for k in steps]
            following = [column(ahead, at + SUB + k) for k in steps]
        core, inverse, pivots = {}, [], []
        roots = jnp.ones((SUB, LANE), F32)
        for i in steps:
            for k in range(i, SUB):
                core[i, k] = splat(columns[k][i : i + 1])
            inverse.append(1.0 / core[i, i])
            roots = jnp.where(rows == i, lax.rsqrt(core[i, i]), roots)
            pivots.append([splat(half[i : i + 1]) for half in state[t0]])
            if i < SUB - 1:
                below = jnp.where(rows > i, columns[i], 0.0)
                for k in range(i + 1, SUB):
                    columns[k] = columns[k] - (below * core[i, k]) * inverse[i]
                ratio = below * inverse[i]
                state[t0] = [half - ratio * p for half, p in zip(state[t0], pivots[i])]
        done.append([half * roots for half in state[t0]])
        limit = min(tiles, PANEL * (t0 // PANEL + 2))
        for t in range(t0 + 1, limit):
            plain, scaled = [], []
            for k in steps:
                value = raw[k] if t == t0 + 1 else column(state[t][0], at + k)
                for i in range(k):
                    value = value - scaled[i] * core[i, k]
                plain.append(value)
                scaled.append(value * inverse[k])
            if t == t0 + 1:
                columns = []
                for j in steps:
                    value = following[j]
                    for k in steps:
                        value = value - scaled[k] * splat(plain[k][j : j + 1])
                    columns.append(value)
            for half in range(2):
                value = state[t][half]
                for k in steps:
                    value = value - scaled[k] * pivots[k][half]
                state[t][half] = value
        if (t0 + 1) % PANEL == 0 and limit < tiles:
            panel = [jnp.concatenate(tile, axis=1) for tile in done[-PANEL:]]
            update = outer(jnp.concatenate(panel, axis=0))
            for t in range(limit, tiles):
                cut = update[SUB * t : SUB * t + SUB]
                state[t] = [state[t][0] - cut[:, :LANE], state[t][1] - cut[:, LANE:]]
    return jnp.concatenate([tile[1] for tile in done], axis=0)


def last_kernel(once, gram, *rest):
    *packs, out, tile, sem = rest
    keep = LANE
    coeffs = once[...]
    cross, far = gram[:keep], gram[keep:]
    cross = exact(exact(coeffs, cross), coeffs, NT)
    far = exact(exact(coeffs, far), coeffs, NT)
    across = lax.broadcasted_iota(jnp.int32, (keep, keep), 1)
    down = lax.broadcasted_iota(jnp.int32, (keep, keep), 0)
    unit = jnp.where(across == down, 1.0, 0.0)
    span_a = unit + exact(cross, cross, NT)
    span_b = cross + exact(cross, far)
    next_a = span_a + exact(span_b, cross, NT)
    next_b = exact(span_a, cross) + exact(span_b, far)
    metric = exact(next_a, span_a, NT) + exact(next_b, span_b, NT)
    spanning = jnp.concatenate([exact(span_a, coeffs), exact(span_b, coeffs)], axis=1)
    turned = exact(spanning.T, eliminate(metric, unit), NT)
    half = LANE // 2
    weights = jnp.concatenate(halves(turned), axis=1)
    weights = jnp.concatenate(
        [weights[half * (k // 2) : half * (k // 2) + half] for k in range(8)], axis=0
    )
    stores = []
    for at, piece in enumerate(packs):
        both = bf(piece[...], weights)
        tile[at] = (both[:, :LANE] + both[:, LANE:]).T
        stores.append(
            pltpu.make_async_copy(
                tile.at[at], out.at[:, pl.ds(at * PIECE, PIECE)], sem.at[at]
            )
        )
        stores[-1].start()
    for store in stores:
        store.wait()


def make_last(packs, once, gram):
    count = len(packs)
    return pl.pallas_call(
        last_kernel,
        out_shape=jax.ShapeDtypeStruct((LANE, count * PIECE), F32),
        in_specs=[VMEM] * (count + 2),
        out_specs=HBM,
        scratch_shapes=[
            pltpu.VMEM((count, LANE, PIECE), F32),
            pltpu.SemaphoreType.DMA((count,)),
        ],
        compiler_params=pltpu.CompilerParams(vmem_limit_bytes=28 << 20),
    )(once, gram, *packs)


def body(source, band_values, offsets):
    total = float(source.shape[1] * lax.axis_size("rows"))
    *packs, once, gram = make_main(source, band_values, offsets, total)
    return make_last(packs, once, gram)


def solution(mesh):
    placed = (P(None, "rows"), P(None, "rows"), P())
    return jax.shard_map(
        body, mesh=mesh, in_specs=placed, out_specs=P(None, "rows"), check_vma=False
    )
```

```python
import functools

import jax
import jax.numpy as jnp
from jax import lax
from jax.experimental import pallas as pl
from jax.experimental.pallas import tpu as pltpu
from jax.sharding import PartitionSpec as P

HB = 128
SUB = 8
LANE = 128
GROUP = 8
PANEL = 4
PIECE = 4 * HB
MESH = pl.DeviceIdType.MESH
VMEM = pl.BlockSpec(memory_space=pltpu.VMEM)
HBM = pl.BlockSpec(memory_space=pltpu.HBM)
NN = (((1,), (0,)), ((), ()))
NT = (((1,), (1,)), ((), ()))
TN = (((0,), (0,)), ((), ()))
F32 = jnp.float32
BF16 = jnp.bfloat16


def bf(a, b, dims=NN):
    return lax.dot_general(a, b, dims, preferred_element_type=F32)


def thirds(value):
    top = value.astype(BF16)
    rest = value - top.astype(F32)
    middle = rest.astype(BF16)
    return top, middle, (rest - middle.astype(F32)).astype(BF16)


def exact(a, b, dims=NN):
    (at,), (bt,) = dims[0]
    a1, a2, a3 = thirds(a)
    b1, b2, b3 = thirds(b)
    left = jnp.concatenate([a1, a1, a2, a2, a1, a3], axis=at)
    return bf(left, jnp.concatenate([b1, b2, b1, b2, b3, b1], axis=bt), dims)


def halves(value):
    high = value.astype(BF16)
    low = (value - high.astype(F32)).astype(BF16)
    return high, low


def block(at, count=1):
    return pl.ds(pl.multiple_of(at * HB, HB), count * HB)


def pack(twice, flip):
    lanes = lax.broadcasted_iota(jnp.int32, twice.shape, 1)
    high = twice.astype(BF16).astype(F32)
    return jnp.where((lanes < LANE // 2) != flip, high, twice - high).astype(BF16)


def pack_columns(part):
    return pack(jnp.concatenate([part, part], axis=0).T, False)


def band_block(values, chosen):
    top, bottom = halves(values.T)
    spread = bf(jnp.concatenate([top, bottom], axis=1), chosen)
    sheared = pltpu.roll(spread, 0, 1, stride=1, stride_axis=0)
    return jnp.concatenate(halves(sheared), axis=1)


def apply_band(bands, skip, z, out, flip, start, count):
    def step(k, _):
        at = start + k
        window = z[block(at, 3)]
        both = bf(bands[at + skip], jnp.concatenate([window, window], axis=0))
        out[block(at)] = pack(both + pltpu.roll(both, LANE // 2, 1), flip)
        return 0

    lax.fori_loop(0, count, step, 0, unroll=count)


def swap(value):
    return pltpu.roll(value, LANE // 2, 1)


def mixed(even, odd):
    lanes = lax.broadcasted_iota(jnp.int32, even.shape, 1)
    first = lanes < LANE // 2
    return jnp.where(first, even, odd), jnp.where(first, odd, even)


class Total:
    def __init__(self, n, refs):
        self.groups = n // GROUP
        me = lax.axis_index("rows")
        self.team, self.seat = me // GROUP, lax.rem(me, GROUP)
        (self.mine, self.got, self.part, self.gotb, self.gathered,
         self.asend, self.arecv, self.bsend, self.brecv, self.csend, self.crecv) = refs

    def mate(self, k):
        return self.team * GROUP + lax.rem(self.seat + k, GROUP)

    def peer(self, k):
        return lax.rem(self.team + k, self.groups) * GROUP + self.seat

    def copy(self, src, dst, send, recv, device):
        return pltpu.make_async_remote_copy(
            src_ref=src, dst_ref=dst, send_sem=send, recv_sem=recv,
            device_id=(device,), device_id_type=MESH,
        )

    def ahead(self, k):
        to = lax.rem(self.seat + k, GROUP)
        return self.copy(
            self.mine.at[to], self.got.at[k], self.asend.at[k], self.arecv.at[k], self.mate(k)
        )

    def across(self, k):
        return self.copy(
            self.part, self.gotb.at[k], self.bsend.at[k], self.brecv.at[k], self.peer(k)
        )

    def back(self, k):
        own = self.gathered.at[self.seat]
        return self.copy(own, own, self.csend.at[k], self.crecv.at[k], self.mate(k))

    def scatter(self, value):
        self.mine[...] = value.reshape(self.mine.shape)
        for k in range(1, GROUP):
            self.ahead(k).start()

    def middle(self):
        summed = self.mine[self.seat]
        for k in range(1, GROUP):
            self.ahead(k).wait_recv()
            summed = summed + self.got[k]
        self.part[...] = summed

        def start(k, _):
            self.across(k).start()
            return 0

        lax.fori_loop(1, self.groups, start, 0)

    def post(self):
        def arrive(k, value):
            self.across(k).wait_recv()
            return value + self.gotb[k]

        self.gathered[self.seat] = lax.fori_loop(1, self.groups, arrive, self.part[...])
        for k in range(1, GROUP):
            self.back(k).start()

    def finish(self):
        for k in range(1, GROUP):
            self.back(k).wait_recv()
        value = self.gathered[...].reshape(GROUP * self.part.shape[0], LANE)
        for k in range(1, GROUP):
            self.ahead(k).wait_send()
            self.back(k).wait_send()

        def sent(k, _):
            self.across(k).wait_send()
            return 0

        lax.fori_loop(1, self.groups, sent, 0)
        return value

    @staticmethod
    def scratch(n, rows):
        groups, share = n // GROUP, rows // GROUP
        vm, dma = pltpu.VMEM, pltpu.SemaphoreType.DMA
        return [
            vm((GROUP, share, LANE), F32), vm((GROUP, share, LANE), F32),
            vm((share, LANE), F32), vm((groups, share, LANE), F32),
            vm((GROUP, share, LANE), F32),
            dma((GROUP,)), dma((GROUP,)), dma((groups,)), dma((groups,)),
            dma((GROUP,)), dma((GROUP,)),
        ]


def main_kernel(
    n, total, source, band, offsets, *rest
):
    pieces = source.shape[1] // PIECE
    packs, (once, gram) = rest[:pieces], rest[pieces : pieces + 2]
    (z0, z1, z2, z3, sv, bv, ov, ls, hs, lb, hb, bands,
     local_sem, hsend, hrecv, *totals) = rest[pieces + 2 :]
    me = lax.axis_index("rows")
    right, left = lax.rem(me + 1, n), lax.rem(me + n - 1, n)
    third = len(totals) // 3
    near, mid, far = [Total(n, totals[third * k : third * k + third]) for k in range(3)]
    local = source.shape[1]
    blocks = local // HB
    deep_s, deep_b = 3 * HB, 2 * HB
    barrier = pltpu.get_barrier_semaphore()

    def greet(device):
        pl.semaphore_signal(barrier, inc=1, device_id=(device,), device_id_type=MESH)

    def greet_peer(k, _):
        greet(near.peer(k))
        return 0

    greet(left)
    greet(right)
    lax.fori_loop(1, near.groups, greet_peer, 0)
    for k in range(1, GROUP):
        greet(near.mate(k))
    whole = pl.ds(0, offsets.shape[1])
    half = local // 2
    cuts = [
        (source, sv, pl.ds(0, deep_s)), (source, sv, pl.ds(local - deep_s, deep_s)),
        (source, sv, pl.ds(deep_s, local - 2 * deep_s)),
        (offsets, ov, whole),
        (band, bv, pl.ds(0, half)), (band, bv, pl.ds(half, half)),
    ]
    loads = [
        pltpu.make_async_copy(src.at[:, where], dst.at[:, where], local_sem.at[index])
        for index, (src, dst, where) in enumerate(cuts)
    ]
    for load in loads:
        load.start()
    for load in loads[:4]:
        load.wait()
    diagonals = band.shape[0]
    places = lax.broadcasted_iota(jnp.int32, (3 * HB, diagonals), 0)
    chosen = jnp.where(places == ov[...] + HB, 1.0, 0.0).T.astype(BF16)
    chosen = jnp.concatenate([chosen, chosen], axis=0)

    def turn(at, _):
        z0[block(at + 3)] = pack_columns(sv[:, block(at)])
        return 0

    lax.fori_loop(0, blocks, turn, 0, unroll=blocks // 2)

    def build(at, _):
        bands[at + 2] = band_block(bv[:, block(at)], chosen)
        return 0

    pl.semaphore_wait(barrier, 2 + GROUP - 1 + near.groups - 1)
    near_low, near_high = pl.ds(0, HB), pl.ds(local - HB, HB)
    far_low, far_high = pl.ds(HB, deep_b), pl.ds(local - deep_s, deep_b)
    own_low, own_high = pl.ds(0, deep_b), pl.ds(local - deep_b, deep_b)
    last, first = pl.ds(deep_b, HB), pl.ds(0, HB)
    moves = (
        (sv.at[:, near_high], ls.at[:, last], right),
        (sv.at[:, near_low], hs.at[:, first], left),
        (sv.at[:, far_high], ls.at[:, own_low], right),
        (sv.at[:, far_low], hs.at[:, far_low], left),
        (bv.at[:, own_high], lb, right),
        (bv.at[:, own_low], hb, left),
    )
    halo = [
        near.copy(src, dst, hsend.at[index], hrecv.at[index], target)
        for index, (src, dst, target) in enumerate(moves)
    ]
    for copy in halo[:4]:
        copy.start()
    loads[4].wait()
    loads[5].wait()
    for copy in halo[4:]:
        copy.start()
    lax.fori_loop(0, blocks, build, 0, unroll=blocks)
    apply_band(bands, 0, z0, z1, True, 3, blocks - 2)

    def edge_source(k):
        part_low = jnp.where(me > 0, ls[:, pl.ds(k * HB, HB)], 0.0)
        z0[pl.ds(k * HB, HB)] = pack_columns(part_low)
        k = 2 - k
        part_high = jnp.where(me < n - 1, hs[:, pl.ds(k * HB, HB)], 0.0)
        z0[pl.ds(3 * HB + local + k * HB, HB)] = pack_columns(part_high)

    def gram_part(*parts):
        even = jnp.concatenate([z0[pl.ds(at * HB + 3 * HB, size * HB)] for at, size in parts], axis=0)
        odd = jnp.concatenate([z1[pl.ds(at * HB + 2 * HB, size * HB)] for at, size in parts], axis=0)
        high, low = mixed(even, odd)
        return bf(high, jnp.concatenate([high, low], axis=1), TN)

    product = gram_part((1, blocks - 2))
    for copy in halo[:2]:
        copy.wait_recv()
    edge_source(2)
    apply_band(bands, 0, z0, z1, True, 2, 1)
    apply_band(bands, 0, z0, z1, True, blocks + 1, 1)
    product = product + gram_part((0, 1), (blocks - 1, 1))
    cross = swap(product[:, LANE:])
    near.scatter(product[:, :LANE] + cross + cross.T)

    for copy in halo[2:]:
        copy.wait_recv()
    for k in range(2):
        edge_source(k)
        part_low = jnp.where(me > 0, lb[:, pl.ds(k * HB, HB)], 0.0)
        part_high = jnp.where(me < n - 1, hb[:, pl.ds(k * HB, HB)], 0.0)
        bands[k] = band_block(part_low, chosen)
        bands[2 + blocks + k] = band_block(part_high, chosen)
    apply_band(bands, 0, z0, z1, True, 0, 2)
    apply_band(bands, 0, z0, z1, True, blocks + 2, 2)
    apply_band(bands, 1, z1, z2, False, 0, blocks + 2)
    half = LANE // 2
    high, low = mixed(z0[pl.ds(3 * HB, local)], z1[pl.ds(2 * HB, local)])

    def gram_rows(z, *others):
        product = bf(z, jnp.concatenate([high, low, *others], axis=1), TN)
        product = product[:half] + product[half:]
        parts = [product[:, k * LANE : k * LANE + LANE] for k in range(2 + len(others))]
        return [parts[0] + swap(parts[1])] + [part + swap(part) for part in parts[2:]]

    inner2 = z2[pl.ds(HB, local)]
    mid.scatter(jnp.concatenate(gram_rows(inner2, inner2), axis=0))
    near.middle()
    apply_band(bands, 2, z2, z3, True, 0, blocks)
    inner3 = z3[...]
    cross, left_part, own = gram_rows(inner3, inner2, inner3)
    lanes = lax.broadcasted_iota(jnp.int32, own.shape, 1)
    far.scatter(jnp.concatenate([cross, jnp.where(lanes < half, left_part, own)], axis=0))
    for index, out in enumerate(packs):
        for at, z in enumerate((z0, z1, z2, z3)):
            where = pl.ds(index * PIECE + (3 - at) * HB, PIECE)
            out[:, at * LANE : (at + 1) * LANE] = z[where]
    mid.middle()
    near.post()
    far.middle()
    gram_one = near.finish() * (1.0 / total)
    mid.post()
    cube = exact(exact(gram_one, gram_one), gram_one)
    turned = eliminate(cube, gram_one)
    far.post()
    spanning = exact(turned, gram_one)
    metric = exact(exact(spanning, gram_one), spanning, NT)
    once[...] = eliminate(metric, spanning)
    upper = mid.finish() * (1.0 / total)
    lower = far.finish() * (1.0 / total)
    gram[...] = jnp.concatenate([upper[:half], lower[:half], upper[half:], lower[half:]], axis=0)
    for copy in halo:
        copy.wait_send()


def make_main(source, band, offsets, total):
    n = lax.axis_size("rows")
    width, local = source.shape
    diagonals = band.shape[0]
    blocks = local // HB
    dma = pltpu.SemaphoreType.DMA
    shape = jax.ShapeDtypeStruct
    vm = pltpu.VMEM
    return pl.pallas_call(
        functools.partial(main_kernel, n, total),
        out_shape=[
            shape((PIECE, 4 * LANE), BF16) for _ in range(local // PIECE)
        ]
        + [shape((LANE, LANE), F32), shape((2 * LANE, LANE), F32)],
        in_specs=[HBM] * 3,
        out_specs=[VMEM] * (local // PIECE + 2),
        scratch_shapes=[
            vm((local + 6 * HB, LANE), BF16),
            vm((local + 4 * HB, LANE), BF16),
            vm((local + 2 * HB, LANE), BF16),
            vm((local, LANE), BF16),
            vm((width, local), F32),
            vm((diagonals, local), F32),
            vm((1, diagonals), jnp.int32),
            vm((width, 3 * HB), F32), vm((width, 3 * HB), F32),
            vm((diagonals, 2 * HB), F32), vm((diagonals, 2 * HB), F32),
            vm((blocks + 4, HB, 6 * HB), BF16),
            dma((6,)), dma((6,)), dma((6,)),
        ]
        + Total.scratch(n, LANE)
        + Total.scratch(n, LANE)
        + Total.scratch(n, LANE),
        compiler_params=pltpu.CompilerParams(
            collective_id=0, has_side_effects=True, vmem_limit_bytes=49 << 20
        ),
    )(source, band, offsets.reshape(1, diagonals))


def splat(value):
    return jnp.broadcast_to(value, (SUB, LANE))


def outer(rows):
    a, b, c = thirds(rows)
    left = jnp.concatenate([part[:, :LANE] for part in (a, a, b, b, a, c)], axis=0)
    return bf(left, jnp.concatenate([a, b, a, b, c, a], axis=0), TN)


def column(value, k):
    return splat(value[:, k : k + 1])


def eliminate(metric, right):
    tiles = metric.shape[0] // SUB
    state = [
        [metric[SUB * t : SUB * t + SUB], right[SUB * t : SUB * t + SUB]] for t in range(tiles)
    ]
    rows = lax.broadcasted_iota(jnp.int32, (SUB, LANE), 0)
    steps = range(SUB)
    columns = [column(state[0][0], k) for k in steps]
    done = []
    for t0 in range(tiles):
        at = SUB * t0
        if t0 + 1 < tiles:
            ahead = state[t0 + 1][0]
            raw = [column(ahead, at + k) for k in steps]
            following = [column(ahead, at + SUB + k) for k in steps]
        core, inverse, pivots = {}, [], []
        roots = jnp.ones((SUB, LANE), F32)
        for i in steps:
            for k in range(i, SUB):
                core[i, k] = splat(columns[k][i : i + 1])
            inverse.append(1.0 / core[i, i])
            roots = jnp.where(rows == i, lax.rsqrt(core[i, i]), roots)
            pivots.append([splat(half[i : i + 1]) for half in state[t0]])
            if i < SUB - 1:
                below = jnp.where(rows > i, columns[i], 0.0)
                for k in range(i + 1, SUB):
                    columns[k] = columns[k] - (below * core[i, k]) * inverse[i]
                ratio = below * inverse[i]
                state[t0] = [half - ratio * p for half, p in zip(state[t0], pivots[i])]
        done.append([half * roots for half in state[t0]])
        limit = min(tiles, PANEL * (t0 // PANEL + 2))
        for t in range(t0 + 1, limit):
            plain, scaled = [], []
            for k in steps:
                value = raw[k] if t == t0 + 1 else column(state[t][0], at + k)
                for i in range(k):
                    value = value - scaled[i] * core[i, k]
                plain.append(value)
                scaled.append(value * inverse[k])
            if t == t0 + 1:
                columns = []
                for j in steps:
                    value = following[j]
                    for k in steps:
                        value = value - scaled[k] * splat(plain[k][j : j + 1])
                    columns.append(value)
            for half in range(2):
                value = state[t][half]
                for k in steps:
                    value = value - scaled[k] * pivots[k][half]
                state[t][half] = value
        if (t0 + 1) % PANEL == 0 and limit < tiles:
            panel = [jnp.concatenate(tile, axis=1) for tile in done[-PANEL:]]
            update = outer(jnp.concatenate(panel, axis=0))
            for t in range(limit, tiles):
                cut = update[SUB * t : SUB * t + SUB]
                state[t] = [state[t][0] - cut[:, :LANE], state[t][1] - cut[:, LANE:]]
    return jnp.concatenate([tile[1] for tile in done], axis=0)


def last_kernel(once, gram, *rest):
    *packs, out, tile, sem = rest
    keep = LANE
    coeffs = once[...]
    across = lax.broadcasted_iota(jnp.int32, (keep, keep), 1)
    down = lax.broadcasted_iota(jnp.int32, (keep, keep), 0)
    cross, far = gram[:keep], gram[keep:]
    far = jnp.where((across >= keep // 2) & (down < keep // 2), far.T, far)
    cross = exact(exact(coeffs, cross, NT), coeffs, NT)
    far = exact(exact(coeffs, far), coeffs, NT)
    unit = jnp.where(across == down, 1.0, 0.0)
    span_a = unit + exact(cross, cross, NT)
    span_b = cross + exact(cross, far)
    next_a = span_a + exact(span_b, cross, NT)
    next_b = exact(span_a, cross) + exact(span_b, far)
    metric = exact(next_a, span_a, NT) + exact(next_b, span_b, NT)
    spanning = jnp.concatenate([exact(span_a, coeffs), exact(span_b, coeffs)], axis=1)
    turned = exact(spanning.T, eliminate(metric, unit), NT)
    half = LANE // 2
    weights = jnp.concatenate(halves(turned), axis=1)
    weights = jnp.concatenate(
        [weights[half * (k // 2) : half * (k // 2) + half] for k in range(8)], axis=0
    )
    stores = []
    for at, piece in enumerate(packs):
        both = bf(piece[...], weights)
        tile[at] = (both[:, :LANE] + both[:, LANE:]).T
        stores.append(
            pltpu.make_async_copy(
                tile.at[at], out.at[:, pl.ds(at * PIECE, PIECE)], sem.at[at]
            )
        )
        stores[-1].start()
    for store in stores:
        store.wait()


def make_last(packs, once, gram):
    count = len(packs)
    return pl.pallas_call(
        last_kernel,
        out_shape=jax.ShapeDtypeStruct((LANE, count * PIECE), F32),
        in_specs=[VMEM] * (count + 2),
        out_specs=HBM,
        scratch_shapes=[
            pltpu.VMEM((count, LANE, PIECE), F32),
            pltpu.SemaphoreType.DMA((count,)),
        ],
        compiler_params=pltpu.CompilerParams(vmem_limit_bytes=28 << 20),
    )(once, gram, *packs)


def body(source, band_values, offsets):
    total = float(source.shape[1] * lax.axis_size("rows"))
    *packs, once, gram = make_main(source, band_values, offsets, total)
    return make_last(packs, once, gram)


def solution(mesh):
    placed = (P(None, "rows"), P(None, "rows"), P())
    return jax.shard_map(
        body, mesh=mesh, in_specs=placed, out_specs=P(None, "rows"), check_vma=False
    )
```
